256 devices in a mesh: rep: 32 (over z_lo, x, core), ep: 8 (over z_hi, y).
Axes of the slice: x: 4, y: 4, z: 8 (z_hi: 2, z_lo: 4; z = z_hi * 4 + z_lo), core: 2. Of those that a mesh axis runs over, the one named last changes fastest.
Arguments:
- tokens: bfloat16 [2, 1024, 4096], P(None, 'ep', 'rep'), may hold values from -6 to 6
- expert_ids: int32 [2, 1024, 2], P(None, 'ep'), may hold values from 0 to 7, all different within a row; in each aligned block of 128 rows (0 to 127, 128 to 255, ..., all dimensions but the last counted through in order) at most 48 rows name the same one
- router_weight: bfloat16 [4096, 8], P('rep'), may hold values from -0.09375 to 0.09375
- w_gate: bfloat16 [8, 4096, 8192], P('ep', None, 'rep'), may hold values from -0.09375 to 0.09375
- w_up: bfloat16 [8, 4096, 8192], P('ep', None, 'rep'), may hold values from -0.09375 to 0.09375
- w_down: bfloat16 [8, 8192, 4096], P('ep', 'rep'), may hold values from -0.0625 to 0.0625
- cotangent: bfloat16 [2, 1024, 4096], P(None, 'ep', 'rep'), may hold values from -6 to 6
Outputs:
- mixed: bfloat16 [2, 1024, 4096], P(None, 'ep', 'rep')
- token_grad: bfloat16 [2, 1024, 4096], P(None, 'ep', 'rep')
- gate_grad: bfloat16 [8, 4096, 8192], P('ep', None, 'rep')
- up_grad: bfloat16 [8, 4096, 8192], P('ep', None, 'rep')
- down_grad: bfloat16 [8, 8192, 4096], P('ep', 'rep')
- router_grad: float32 [4096, 8], P('rep')
The draws below stay inside these ranges and needn't reach their ends.
Inputs may be any that keep to these rules, and one draw needn't show every extreme that they name: `expert_ids`: each row names 2 different experts. Among the 128 rows of one index of ep in one microbatch no expert is named by more than 48 rows, and in every draw some expert is named by exactly 48 of them.
All inputs are finite; a program needn't handle non-finite values.
Results may differ from the reference program's by a relative error of at most 0.025.
Values may be sent and summed in bfloat16 or wider, within the bound.
A program may use at most 128 MiB of HBM per device.

```python
import math
import jax
import jax.numpy as jnp
import numpy as np
from jax import lax

D = 4096
FF = 8192
EXPERTS = 8
TOP = 2
TOK_DEV = 128
MICRO = 2
CAP = 48
TOKENS = 1024
N_REP = 32
N_EP = 8


def shard_levels(own_key, shape, shards, low, largest):
    factor_of, own = 1.0, jax.random.fold_in(own_key, 6)
    for axis_at, blocks in shards:
        draws = jnp.exp(jax.random.uniform(jax.random.fold_in(own, axis_at), (blocks,), jnp.float32, low / len(shards), largest / len(shards)))
        factor_of = factor_of * jnp.repeat(draws, shape[axis_at] // blocks).reshape([-1 if axis == axis_at else 1 for axis in range(len(shape))])
    return factor_of


def shared_out(rng, own, number, rows, number_of, top, reach, skew):
    sequence = jax.random.permutation(rng, number_of)
    packed, ordinary = shares(number_of, rows * top, reach, skew, True), shares(number_of, rows * top, reach, skew, False)
    places = jnp.arange(number_of)

    def named(tallies, turn):
        used = int((tallies > 0).sum())
        fixed = max(1, used // 4)
        passed = fixed + (places - fixed + turn * (used - fixed)) % max(1, number_of - fixed)
        return jnp.zeros((number_of,), jnp.int32).at[sequence[jnp.where(places < fixed, places, passed)]].set(jnp.asarray(tallies, jnp.int32))

    tallies = jnp.where(number % 4 == 0, named(packed, number // 4), named(ordinary, number - number // 4 - 1))
    mixed = jax.random.permutation(jax.random.fold_in(own, 3), number_of)
    donor, sink = mixed[0:number_of // 2 * 2:2], mixed[1:number_of // 2 * 2:2]
    room = jnp.minimum(tallies[donor] - 1, reach - tallies[sink]) // 2
    room = jnp.where((donor == sequence[0]) | (sink == sequence[0]) | (tallies[sink] == 0), 0, jnp.maximum(room, 0))
    passed = jax.random.randint(jax.random.fold_in(own, 4), (number_of // 2,), 0, 1 << 20) % (room + 1)
    tallies = tallies.at[donor].add(-passed).at[sink].add(passed)
    members = jnp.searchsorted(jnp.cumsum(tallies), jnp.arange(rows * top), side="right").astype(jnp.int32)
    listing = members.reshape(top, rows).T
    listing = listing[jax.random.permutation(jax.random.fold_in(own, 1), rows)]
    turn = jax.random.randint(jax.random.fold_in(own, 2), (rows, 1), 0, top)
    return jnp.take_along_axis(listing, (jnp.arange(top)[None, :] + turn) % top, axis=1)


def shares(number_of, total, reach, skew, full):
    weights = [(1 << 20) // math.isqrt(standing ** skew) + 1 for standing in range(1, number_of + 1)]
    largest = reach if full else min(reach, max(-(-total // number_of), total * weights[0] // sum(weights)))
    least = 1 if total - largest >= number_of - 1 else 0
    holding, rest = [largest] + [least] * (number_of - 1), total - largest - least * (number_of - 1)
    while rest > 0:
        candidates = [i for i in range(1, number_of) if holding[i] < largest] or [i for i in range(1, number_of) if holding[i] < reach]
        whole, budget = sum([weights[i] for i in candidates]), rest
        for i in candidates:
            addition = min(reach - holding[i], max(1, budget * weights[i] // whole), rest)
            holding[i] = holding[i] + addition
            rest = rest - addition
    return np.array(holding)


def normal_values(rng, dims, scale, bound, shards=(), kind=jnp.bfloat16):
    entries = jax.random.normal(rng, dims, jnp.float32) * scale
    if len(shards) > 0:
        entries = shard_levels(rng, dims, shards, -0.22, 0.18) * entries
    return jnp.clip(entries, min=-bound, max=bound).astype(kind)


def setup_inputs(seed: int = 0) -> dict:
    splits = jax.random.split(jax.random.key(seed), 8)
    tokens = normal_values(splits[0], (MICRO, TOKENS, D), 1.0, 6.0, ((1, 8), (2, 32)))
    expert_ids_keys = jax.random.split(jax.random.fold_in(splits[1], 1), MICRO * TOKENS // TOK_DEV)
    expert_ids_turns = jax.random.permutation(jax.random.fold_in(splits[1], 3), MICRO * TOKENS // TOK_DEV)
    expert_ids = jax.vmap(lambda own, number: shared_out(jax.random.fold_in(splits[1], 2), own, number, TOK_DEV, EXPERTS, TOP, CAP, 2))(expert_ids_keys, expert_ids_turns).reshape((MICRO, TOKENS, TOP))
    router_weight = normal_values(splits[2], (D, EXPERTS), D ** -0.5, 0.09375, ((0, 32),))
    w_gate = normal_values(splits[3], (EXPERTS, D, FF), D ** -0.5, 0.09375, ((0, 8), (2, 32)))
    w_up = normal_values(splits[4], (EXPERTS, D, FF), D ** -0.5, 0.09375, ((0, 8), (2, 32)))
    w_down = normal_values(splits[5], (EXPERTS, FF, D), FF ** -0.5, 0.0625, ((0, 8), (1, 32)))
    cotangent = normal_values(splits[6], (MICRO, TOKENS, D), 1.0, 6.0, ((1, 8), (2, 32)))
    return dict(tokens=tokens, expert_ids=expert_ids, router_weight=router_weight, w_gate=w_gate, w_up=w_up, w_down=w_down, cotangent=cotangent)


def positions(route_ids):
    hits = route_ids[:, :, None] == jnp.arange(EXPERTS, dtype=jnp.int32)[None, None, :]
    per_token = jnp.sum(hits.astype(jnp.int32), axis=1)
    before = jnp.cumsum(per_token, axis=0) - per_token
    return jnp.sum(jnp.where(hits, before[:, None, :], 0), axis=2).astype(jnp.int32)


def widen(value):
    return lax.optimization_barrier(value.astype(jnp.bfloat16)).astype(jnp.float32)


def expert_forward(rows_in, gate_w, up_w):
    pre_gate = jnp.dot(rows_in, gate_w, preferred_element_type=jnp.float32)
    pre_up = jnp.dot(rows_in, up_w, preferred_element_type=jnp.float32)
    hidden = (jax.nn.silu(pre_gate) * pre_up).astype(jnp.bfloat16)
    return pre_gate, pre_up, hidden


def grouped_down(hidden, down_w):
    group = FF // N_REP
    slots = hidden.shape[0]
    parts_h = hidden.reshape(slots, N_REP, group).transpose(1, 0, 2)
    parts_w = down_w.reshape(N_REP, group, D)

    def add(total, pair):
        return total + widen(jnp.dot(pair[0], pair[1], preferred_element_type=jnp.float32)), None

    total, _ = lax.scan(add, jnp.zeros((slots, D), jnp.float32), (parts_h, parts_w))
    return total.astype(jnp.bfloat16)


def grouped_in(gate_part, up_part, gate_w, up_w):
    group = FF // N_REP
    slots = gate_part.shape[0]
    parts_g = gate_part.reshape(slots, N_REP, group).transpose(1, 0, 2)
    parts_u = up_part.reshape(slots, N_REP, group).transpose(1, 0, 2)
    weights_g = gate_w.reshape(D, N_REP, group).transpose(1, 0, 2)
    weights_u = up_w.reshape(D, N_REP, group).transpose(1, 0, 2)

    def add(total, items):
        term = jnp.dot(items[0], items[2].T, preferred_element_type=jnp.float32)
        term = term + jnp.dot(items[1], items[3].T, preferred_element_type=jnp.float32)
        return total + widen(term), None

    total, _ = lax.scan(add, jnp.zeros((slots, D), jnp.float32), (parts_g, parts_u, weights_g, weights_u))
    return total.astype(jnp.bfloat16)


def reference(tokens, expert_ids, router_weight, w_gate, w_up, w_down, cotangent):
    slot_count = N_EP * CAP
    source = jnp.arange(TOKENS, dtype=jnp.int32) // TOK_DEV
    plans = []
    inputs = []
    for step in range(MICRO):
        route_ids = expert_ids[step].astype(jnp.int32)
        places = jax.vmap(positions)(route_ids.reshape(N_EP, TOK_DEV, TOP)).reshape(TOKENS, TOP)
        row_ids = (source[:, None] * CAP + places).astype(jnp.int32)
        values = jnp.broadcast_to(tokens[step][:, None, :], (TOKENS, TOP, D))
        inputs.append(jnp.zeros((EXPERTS, slot_count, D), jnp.bfloat16).at[route_ids, row_ids].set(values))
        plans.append((route_ids, row_ids))
    expert_in = jnp.stack(inputs, axis=1)

    def forward_one(items):
        rows_all, gate_w, up_w, down_w = items
        outs = []
        for step in range(MICRO):
            pre_gate, pre_up, hidden = expert_forward(rows_all[step], gate_w, up_w)
            outs.append(grouped_down(hidden, down_w))
        return jnp.stack(outs)

    expert_out = lax.map(forward_one, (expert_in, w_gate, w_up, w_down))
    mixed = []
    cots = []
    logit_grads = []
    router_grad = jnp.zeros((D, EXPERTS), jnp.float32)
    for step in range(MICRO):
        route_ids, row_ids = plans[step]
        logits = jnp.dot(tokens[step], router_weight, preferred_element_type=jnp.float32)
        hits = route_ids[:, :, None] == jnp.arange(EXPERTS, dtype=jnp.int32)[None, None, :]
        chosen = jnp.sum(jnp.where(hits, logits[:, None, :], 0.0), axis=2)
        spread = chosen[:, 0] - chosen[:, 1]
        gates = jnp.stack([jax.nn.sigmoid(spread), jax.nn.sigmoid(-spread)], axis=1)
        pairs = expert_out[:, step][route_ids, row_ids].astype(jnp.float32)
        mixed.append((gates[:, 0, None] * pairs[:, 0] + gates[:, 1, None] * pairs[:, 1]).astype(jnp.bfloat16))
        cot = cotangent[step].astype(jnp.float32)
        gate_dots = jnp.sum(cot[:, None, :] * pairs, axis=2)
        delta = (gate_dots[:, 0] - gate_dots[:, 1]) * gates[:, 0] * gates[:, 1]
        logit_grad = delta[:, None] * (hits[:, 0].astype(jnp.float32) - hits[:, 1].astype(jnp.float32))
        logit_grads.append(logit_grad)
        router_grad = router_grad + jnp.dot(tokens[step].astype(jnp.float32).T, logit_grad, precision=lax.Precision.HIGHEST)
        cot_pairs = (gates[:, :, None] * cot[:, None, :]).astype(jnp.bfloat16)
        cots.append(jnp.zeros((EXPERTS, slot_count, D), jnp.bfloat16).at[route_ids, row_ids].set(cot_pairs))
    expert_cot = jnp.stack(cots, axis=1)

    def backward_one(items):
        rows_all, cots_all, gate_w, up_w, down_w = items
        gate_acc = jnp.zeros((D, FF), jnp.float32)
        up_acc = jnp.zeros((D, FF), jnp.float32)
        down_acc = jnp.zeros((FF, D), jnp.float32)
        grads_in = []
        for step in range(MICRO):
            rows_in = rows_all[step]
            cot_rows = cots_all[step]
            pre_gate, pre_up, hidden = expert_forward(rows_in, gate_w, up_w)
            hidden_grad = jnp.dot(cot_rows, down_w.T, preferred_element_type=jnp.float32)
            gate_sig = jax.nn.sigmoid(pre_gate)
            gate_act = pre_gate * gate_sig
            pre_gate_grad = (hidden_grad * pre_up * (gate_sig * (1.0 + pre_gate * (1.0 - gate_sig)))).astype(jnp.bfloat16)
            pre_up_grad = (hidden_grad * gate_act).astype(jnp.bfloat16)
            down_acc = down_acc + jnp.dot(hidden.T, cot_rows, preferred_element_type=jnp.float32)
            gate_acc = gate_acc + jnp.dot(rows_in.T, pre_gate_grad, preferred_element_type=jnp.float32)
            up_acc = up_acc + jnp.dot(rows_in.T, pre_up_grad, preferred_element_type=jnp.float32)
            grads_in.append(grouped_in(pre_gate_grad, pre_up_grad, gate_w, up_w))
        return gate_acc.astype(jnp.bfloat16), up_acc.astype(jnp.bfloat16), down_acc.astype(jnp.bfloat16), jnp.stack(grads_in)

    gate_grad, up_grad, down_grad, expert_in_grad = lax.map(backward_one, (expert_in, expert_cot, w_gate, w_up, w_down))
    token_grad = []
    for step in range(MICRO):
        route_ids, row_ids = plans[step]
        pairs = expert_in_grad[:, step][route_ids, row_ids].astype(jnp.float32)
        router_in = jnp.dot(logit_grads[step], router_weight.astype(jnp.float32).T, precision=lax.Precision.HIGHEST)
        token_grad.append((pairs[:, 0] + pairs[:, 1] + router_in).astype(jnp.bfloat16))
    return jnp.stack(mixed), jnp.stack(token_grad), gate_grad, up_grad, down_grad, router_grad
```

```python
import jax
import jax.numpy as jnp
from jax import lax
from jax.experimental import pallas as pl
from jax.experimental.pallas import tpu as pltpu
from jax.sharding import Mesh
from jax.sharding import PartitionSpec as P

MESH = pl.DeviceIdType.MESH
REP = ("zl", "x", "c")
EP = ("zh", "y")
F32 = jnp.float32
BF = jnp.bfloat16
CAP = 48
ROWS = 384
BLK = 128
HID = 256
PEERS = [(dz, dy) for dz in range(2) for dy in range(4) if dz or dy]


def rem(value, n):
    return lax.rem(value, jnp.int32(n))


def wait(ref, sem):
    pltpu.make_async_copy(ref, ref, sem).wait()


def dot(a, b):
    return jnp.dot(a, b, preferred_element_type=F32)


def dot_tn(a, b):
    return lax.dot_general(a, b, (((0,), (0,)), ((), ())), preferred_element_type=F32)


def dot_nt(a, b):
    return lax.dot_general(a, b, (((1,), (1,)), ((), ())), preferred_element_type=F32)


def iota(rows, lanes, dim):
    return lax.broadcasted_iota(jnp.int32, (rows, lanes), dim).astype(F32)


def to_row(col):
    n = col.shape[0]
    return jnp.sum(jnp.where(iota(n, BLK, 0) == iota(n, BLK, 1), col, 0.0), axis=0, keepdims=True)


def to_col(row, n):
    return jnp.sum(jnp.where(iota(n, BLK, 0) == iota(n, BLK, 1), row, 0.0), axis=1, keepdims=True)


def tile_of(rows):
    sub = iota(8, BLK, 0)
    return jnp.where(sub == 0.0, rows[0], 0.0) + jnp.where(sub == 1.0, rows[1], 0.0)


def sigmoid(v):
    return 1.0 / (1.0 + jnp.exp(-v))


def kernel(
    tok, cot, ids, rwt, wg_h, wu_h, wd_h,
    mixed, tgrad, gg_h, ug_h, dg_h, rg,
    G, wg, wu, wd, WgH, WuH, WdH, snd, AG, AU, HG, HC, PG, PU, HS, gcol, dcol,
    Pt, FX, XL, XR, zs, zr, zo, fin, ret, slots, gates, dmat, arS, arR, gts, gtr, dts, dtr, rgs, rgr,
    w_l, w_s, w_r, a_s, a_r, z_s, z_r, x_s, xl_r, xr_r, f_r, d_s, d_r, h_s, h_r,
    rx_s, rf_r, rl_r, rr_r, rz_s, rz_r, b_s, b_r, ar_s, ar_r, gt_s, gt_r, dt_s, dt_r, rg_s, rg_r, o_s,
):
    zl = lax.axis_index("zl")
    x = lax.axis_index("x")
    c = lax.axis_index("c")
    zh = lax.axis_index("zh")
    y = lax.axis_index("y")
    right, left, far = rem(x + 1, 4), rem(x + 3, 4), rem(x + 2, 4)
    e = zh * 4 + y
    oc = 1 - c
    r = zl * 8 + x * 2 + c

    def send(src, dst, ss, rs, dev):
        pltpu.make_async_remote_copy(
            src_ref=src, dst_ref=dst, send_sem=ss, recv_sem=rs, device_id=dev, device_id_type=MESH
        ).start()

    def lanes(index, width=BLK):
        return pl.ds(pl.multiple_of(index * width, width), width)

    def feat(zl_, x_, c_):
        return zl_ * 8 + x_ * 2 + c_

    def col(arr, zl_, x_):
        return G.at[arr, :, lanes(feat(zl_, x_, c))]

    def cap(index):
        return pl.ds(pl.multiple_of(index * CAP, 16), CAP)

    mine = lanes(c, HID)

    pltpu.make_async_copy(wg_h, wg, w_l.at[0]).start()
    pltpu.make_async_copy(wu_h, wu, w_l.at[1]).start()
    pltpu.make_async_copy(wd_h, wd, w_l.at[2]).start()

    @pl.loop(0, 16)
    def _(b):
        at = feat(b // 4, b % 4, c)
        pltpu.make_async_copy(wg_h.at[lanes(at), :], WgH.at[lanes(b), mine], w_l.at[3]).start()
        pltpu.make_async_copy(wu_h.at[lanes(at), :], WuH.at[lanes(b), mine], w_l.at[4]).start()
        pltpu.make_async_copy(wd_h.at[:, lanes(at)], WdH.at[mine, lanes(b)], w_l.at[5]).start()

    barrier = pltpu.get_barrier_semaphore()
    pl.semaphore_signal(barrier, inc=1, device_id={"c": oc}, device_id_type=MESH)
    for j in range(1, 4):
        pl.semaphore_signal(barrier, inc=1, device_id={"x": rem(x + j, 4)}, device_id_type=MESH)
        pl.semaphore_signal(barrier, inc=1, device_id={"zl": rem(zl + j, 4)}, device_id_type=MESH)
    for dz, dy in PEERS:
        dev = {"zh": rem(zh + dz, 2), "y": rem(y + dy, 4)}
        pl.semaphore_signal(barrier, inc=1, device_id=dev, device_id_type=MESH)

    sub, lane = iota(BLK, BLK, 0), iota(BLK, BLK, 1)

    def hits(m):
        both = ids[m].astype(F32)
        first, second = both[:, 0:1], both[:, 1:2]
        return first, second, jnp.where(first == lane, 1.0, 0.0), jnp.where(second == lane, 1.0, 0.0)

    spread = []
    for m in range(2):
        first, second, h0, h1 = hits(m)
        tri = jnp.where(lane < sub, 1.0, 0.0).astype(BF)
        before = dot(tri, (h0 + h1).astype(BF))
        s0 = first * float(CAP) + jnp.sum(h0 * before, axis=1, keepdims=True)
        s1 = second * float(CAP) + jnp.sum(h1 * before, axis=1, keepdims=True)
        slots[m, 0] = jnp.broadcast_to(s0, (BLK, BLK))
        slots[m, 1] = jnp.broadcast_to(s1, (BLK, BLK))
        at = iota(ROWS, BLK, 0)
        match = jnp.where((at == to_row(s0)) | (at == to_row(s1)), 1.0, 0.0).astype(BF)
        snd[2 * m] = dot(match, tok[m]).astype(BF)
        snd[2 * m + 1] = dot(match, cot[m]).astype(BF)
        diff = dot((h0 - h1).astype(BF), rwt[...])
        dmat[m] = diff
        spread.append(to_row(jnp.sum(tok[m].astype(F32) * diff, axis=1, keepdims=True)))
    arS[0, 0] = tile_of(spread)
    for arr in range(4):
        G[arr, cap(e), lanes(r)] = snd[arr, cap(e), :]

    pl.semaphore_wait(barrier, 14)

    for arr in range(4):
        for dz, dy in PEERS:
            tz, ty = rem(zh + dz, 2), rem(y + dy, 4)
            send(snd.at[arr, cap(tz * 4 + ty), :], G.at[arr, cap(e), lanes(r)],
                 a_s.at[arr], a_r.at[arr], {"zh": tz, "y": ty})

    def ar_core(k):
        send(arS.at[k, 0], arR.at[k, 0], ar_s.at[k, 0], ar_r.at[k, 0], {"c": oc})

    def ar_x(k):
        wait(arR.at[k, 0], ar_r.at[k, 0])
        arS[k, 1] = arS[k, 0] + arR[k, 0]
        for j in range(1, 4):
            send(arS.at[k, 1], arR.at[k, j], ar_s.at[k, 1], ar_r.at[k, j], {"x": rem(x + j, 4)})

    def ar_z(k):
        total = arS[k, 1]
        for j in range(1, 4):
            wait(arR.at[k, j], ar_r.at[k, j])
            total = total + arR[k, j]
        arS[k, 2] = total
        for j in range(1, 4):
            send(arS.at[k, 2], arR.at[k, 3 + j], ar_s.at[k, 2], ar_r.at[k, 3 + j], {"zl": rem(zl + j, 4)})

    def ar_end(k):
        total = arS[k, 2]
        for j in range(1, 4):
            wait(arR.at[k, 3 + j], ar_r.at[k, 3 + j])
            total = total + arR[k, 3 + j]
        return total

    ar_core(0)

    @pl.loop(0, 16)
    def _(b):
        at = feat(b // 4, b % 4, oc)
        send(wg_h.at[lanes(at), :], WgH.at[lanes(b), mine], w_s.at[0], w_r.at[0], {"c": oc})
        send(wu_h.at[lanes(at), :], WuH.at[lanes(b), mine], w_s.at[1], w_r.at[1], {"c": oc})
        send(wd_h.at[:, lanes(at)], WdH.at[mine, lanes(b)], w_s.at[2], w_r.at[2], {"c": oc})

    def spread_block(arr, zl_, j):
        here = col(arr, zl_, x)
        send(here, here, x_s.at[arr], xl_r.at[arr, j], {"x": right})
        send(here, here, x_s.at[arr], xr_r.at[arr, j], {"x": left})
        send(here, here, d_s.at[arr], d_r.at[arr], {"c": oc})

    def stage_a(arr):
        wait(snd.at[arr, 0:336, :], a_r.at[arr])
        here = col(arr, zl, x)
        for j in range(1, 4):
            send(here, here, z_s.at[arr], z_r.at[arr, j - 1], {"zl": rem(zl + 4 - j, 4)})
        spread_block(arr, zl, 0)

    def stage_b(arr):
        for j in range(1, 4):
            zj = rem(zl + j, 4)
            wait(col(arr, zj, x), z_r.at[arr, j - 1])
            spread_block(arr, zj, j)

    def stage_c(arr):
        for j in range(4):
            zj = rem(zl + j, 4)
            here = col(arr, zj, left)
            wait(here, xl_r.at[arr, j])
            if j % 2 == 0:
                send(here, here, x_s.at[arr], f_r.at[arr, j], {"x": right})
            send(here, here, d_s.at[arr], d_r.at[arr], {"c": oc})
            here = col(arr, zj, right)
            wait(here, xr_r.at[arr, j])
            if j % 2 == 1:
                send(here, here, x_s.at[arr], f_r.at[arr, j], {"x": left})
            send(here, here, d_s.at[arr], d_r.at[arr], {"c": oc})

    def stage_d(arr):
        for j in range(4):
            here = col(arr, rem(zl + j, 4), far)
            wait(here, f_r.at[arr, j])
            send(here, here, d_s.at[arr], d_r.at[arr], {"c": oc})

    def stage_e(arr):
        wait(G.at[arr, :, 0:2048], d_r.at[arr])

    def make_gates():
        total = ar_end(0)
        for m in range(2):
            diff = to_col(total[m : m + 1, :], BLK)
            gates[m, 0] = jnp.broadcast_to(sigmoid(diff), (BLK, BLK))
            gates[m, 1] = jnp.broadcast_to(sigmoid(-diff), (BLK, BLK))

        @pl.loop(0, 8)
        def _(ex):
            at = lane + (ex * CAP).astype(F32)
            rows = []
            for m in range(2):
                picked = jnp.where(slots[m, 0] == at, gates[m, 0], 0.0)
                picked = picked + jnp.where(slots[m, 1] == at, gates[m, 1], 0.0)
                rows.append(jnp.sum(picked, axis=0, keepdims=True))
            gts[ex] = tile_of(rows)

        gtr[e] = gts[e]
        for n, (dz, dy) in enumerate(PEERS):
            tz, ty = rem(zh + dz, 2), rem(y + dy, 4)
            send(gts.at[tz * 4 + ty], gtr.at[e], gt_s.at[0], gt_r.at[0], {"zh": tz, "y": ty})

    def take_gates():
        wait(gts.at[0:7], gt_r.at[0])

        @pl.loop(0, 8)
        def _(s):
            tile = gtr[s]
            for m in range(2):
                gcol[m, cap(s), :] = jnp.broadcast_to(to_col(tile[m : m + 1, :], CAP), (CAP, BLK))

    def pre(m):
        AG[...] = jnp.zeros_like(AG)
        AU[...] = jnp.zeros_like(AU)

        @pl.loop(0, 4)
        def _(k):
            rows = G[2 * m, :, lanes(k, 1024)]
            AG[...] += dot(rows, wg[lanes(k, 1024), :])
            AU[...] += dot(rows, wu[lanes(k, 1024), :])

    def back(m):
        HG[...] = jnp.zeros_like(HG)

        @pl.loop(0, 4)
        def _(k):
            HG[...] += dot_nt(G[2 * m + 1, :, lanes(k, 1024)], wd[:, lanes(k, 1024)])

        @pl.loop(0, 6)
        def _(i):
            rows = lanes(i, 64)
            pg, pu, hr = AG[rows, :], AU[rows, :], HG[rows, :]
            g = gcol[m, rows, 0:1]
            sig = sigmoid(pg)
            act = pg * sig
            hb = (act * pu).astype(BF)
            hw = hb.astype(F32)
            dcol[m, rows, :] = jnp.broadcast_to(jnp.sum(hw * hr, axis=1, keepdims=True), (64, BLK))
            hs = hr * g
            HC[m, rows, mine] = hb
            PG[m, rows, mine] = (hs * pu * (sig * (1.0 + pg * (1.0 - sig)))).astype(BF)
            PU[m, rows, mine] = (hs * act).astype(BF)
            HS[m, rows, :] = (hw * g).astype(BF)

        for n, buf in enumerate((HC, PG, PU)):
            send(buf.at[m, :, mine], buf.at[m, :, mine], h_s.at[m, n], h_r.at[m, n], {"c": oc})

    def part(a, zl_, x_):
        return Pt.at[a, :, lanes(zl_ * 4 + x_)]

    def first_sends(a, zp, parity, q):
        if parity == 0:
            send(part(a, zp, far), FX.at[a, zp], rx_s.at[a], rf_r.at[a, zp], {"x": right})
            send(part(a, zp, left), XR.at[a, zp], rx_s.at[a], rr_r.at[a, zp], {"x": left})
        else:
            send(part(a, zp, far), FX.at[a, zp], rx_s.at[a], rf_r.at[a, zp], {"x": left})
            send(part(a, zp, right), XL.at[a, zp], rx_s.at[a], rl_r.at[a, zp], {"x": right})

    def outs(m):
        a = 2 * m
        wait(HC.at[m, :, 0:HID], h_r.at[m, 0])

        @pl.loop(0, 2)
        def _(q):
            for parity in range(2):
                zp = q * 2 + parity
                Pt[a, :, lanes(zp, 512)] = dot(HC[m], WdH[:, lanes(zp, 512)]).astype(BF)
            for parity in range(2):
                first_sends(a, q * 2 + parity, parity, q)

    def ins(m):
        a = 2 * m + 1
        wait(PG.at[m, :, 0:HID], h_r.at[m, 1])
        wait(PU.at[m, :, 0:HID], h_r.at[m, 2])

        @pl.loop(0, 2)
        def _(q):
            for parity in range(2):
                zp = q * 2 + parity
                Pt[a, :, lanes(zp, 512)] = (
                    dot_nt(PG[m], WgH[lanes(zp, 512), :]) + dot_nt(PU[m], WuH[lanes(zp, 512), :])
                ).astype(BF)
            for parity in range(2):
                first_sends(a, q * 2 + parity, parity, q)

    def second_sends(a):
        for zp in range(4):
            wait(FX.at[a, zp], rf_r.at[a, zp])
            tx = right if zp % 2 == 0 else left
            where = lanes(zp * 4 + tx)
            Pt[a, :, where] = (Pt[a, :, where].astype(F32) + FX[a, zp].astype(F32)).astype(BF)
            if zp % 2 == 0:
                send(part(a, zp, tx), XL.at[a, zp], rx_s.at[a], rl_r.at[a, zp], {"x": right})
            else:
                send(part(a, zp, tx), XR.at[a, zp], rx_s.at[a], rr_r.at[a, zp], {"x": left})

    def third_sends(a):
        for j in (1, 2, 3, 0):
            zp = rem(zl + j, 4)
            wait(XL.at[a, zp], rl_r.at[a, zp])
            wait(XR.at[a, zp], rr_r.at[a, zp])
            total = Pt[a, :, lanes(zp * 4 + x)].astype(F32)
            total = total + XL[a, zp].astype(F32) + XR[a, zp].astype(F32)
            if j == 0:
                zo[a] = total
            else:
                zs[a, j - 1] = total.astype(BF)
                send(zs.at[a, j - 1], zr.at[a, j - 1], rz_s.at[a], rz_r.at[a, j - 1], {"zl": zp})

    def finish(a):
        total = zo[a]
        for j in range(3):
            wait(zr.at[a, j], rz_r.at[a, j])
            total = total + zr[a, j].astype(F32)
        fin[a] = total.astype(BF)
        ret[a, cap(e), :] = fin[a, cap(e), :]
        for dz, dy in PEERS:
            tz, ty = rem(zh + dz, 2), rem(y + dy, 4)
            send(fin.at[a, cap(tz * 4 + ty), :], ret.at[a, cap(e), :], b_s.at[a], b_r.at[a], {"zh": tz, "y": ty})

    def send_dots():
        @pl.loop(0, 8)
        def _(s):
            dts[s] = tile_of([to_row(dcol[m, cap(s), :]) for m in range(2)])

        dtr[e] = dts[e]
        for dz, dy in PEERS:
            tz, ty = rem(zh + dz, 2), rem(y + dy, 4)
            send(dts.at[tz * 4 + ty], dtr.at[e], dt_s.at[0], dt_r.at[0], {"zh": tz, "y": ty})

    def take_dots():
        wait(dts.at[0:7], dt_r.at[0])
        rows = []
        for m in range(2):
            total = jnp.zeros((BLK, BLK), F32)
            for ex in range(8):
                at = lane + float(ex * CAP)
                row = dtr[ex][m : m + 1, :]
                total = total + jnp.where(slots[m, 0] == at, row, 0.0) - jnp.where(slots[m, 1] == at, row, 0.0)
            rows.append(to_row(jnp.sum(total, axis=1, keepdims=True)))
        arS[1, 0] = tile_of(rows)
        ar_core(1)

    def weight_grads(lo, hi):
        @pl.loop(lo, hi)
        def _(i):
            at = lanes(i, 512)
            t0, t1 = G[0, :, at], G[2, :, at]
            wg[at, :] = (dot_tn(t0, PG[0, :, mine]) + dot_tn(t1, PG[1, :, mine])).astype(BF)
            wu[at, :] = (dot_tn(t0, PU[0, :, mine]) + dot_tn(t1, PU[1, :, mine])).astype(BF)
            wd[:, at] = (dot_tn(HS[0], G[1, :, at]) + dot_tn(HS[1], G[3, :, at])).astype(BF)

    stage_a(0)
    ar_x(0)
    stage_a(1)
    stage_b(0)
    ar_z(0)
    stage_a(2)
    stage_a(3)
    stage_b(1)
    make_gates()
    stage_c(0)
    stage_b(2)
    stage_c(1)
    stage_d(0)
    stage_b(3)
    stage_e(0)
    for k, buf in enumerate((wg, wu, wd)):
        wait(buf, w_l.at[k])
    for k, half in enumerate((WgH.at[:, 0:HID], WuH.at[:, 0:HID], WdH.at[0:HID, :])):
        wait(half, w_l.at[3 + k])
        wait(half, w_r.at[k])
    pre(0)
    stage_c(2)
    stage_d(1)
    stage_e(1)
    take_gates()
    back(0)
    outs(0)
    stage_c(3)
    ins(0)
    stage_d(2)
    stage_e(2)
    pre(1)
    second_sends(0)
    stage_d(3)
    stage_e(3)
    back(1)
    second_sends(1)
    outs(1)
    ins(1)
    send_dots()
    third_sends(0)
    third_sends(1)
    finish(0)
    take_dots()
    weight_grads(0, 4)
    second_sends(2)
    second_sends(3)
    ar_x(1)
    finish(1)
    weight_grads(4, 8)
    for k, (buf, out) in enumerate(((wg, gg_h), (wu, ug_h), (wd, dg_h))):
        pltpu.make_async_copy(buf, out, o_s.at[k]).start()
    ar_z(1)
    third_sends(2)
    third_sends(3)

    total = ar_end(1)
    share = jnp.zeros((BLK, BLK), F32)
    deltas = []
    for m in range(2):
        _, _, h0, h1 = hits(m)
        delta = to_col(total[m : m + 1, :], BLK) * gates[m, 0] * gates[m, 1]
        deltas.append(delta)
        share = share + lax.dot_general(
            delta * (h0 - h1), tok[m].astype(F32), (((0,), (0,)), ((), ())),
            preferred_element_type=F32, precision=lax.Precision.HIGHEST,
        )
    rgs[...] = share[0:8, :]
    for n, (dz, dy) in enumerate(PEERS):
        tz, ty = rem(zh + dz, 2), rem(y + dy, 4)
        send(rgs, rgr.at[n], rg_s.at[0], rg_r.at[n], {"zh": tz, "y": ty})
    finish(2)
    finish(3)

    for m in range(2):
        a = 2 * m
        wait(ret.at[a, 0:336, :], b_r.at[a])
        wait(ret.at[a + 1, 0:336, :], b_r.at[a + 1])
        one = jnp.zeros((BLK, BLK), F32)
        two = jnp.zeros((BLK, BLK), F32)
        grad = deltas[m] * dmat[m]
        for q in range(3):
            at = lane + float(q * BLK)
            p0 = jnp.where(slots[m, 0] == at, 1.0, 0.0)
            p1 = jnp.where(slots[m, 1] == at, 1.0, 0.0)
            rows = ret[a, q * BLK : (q + 1) * BLK, :]
            one = one + dot(p0.astype(BF), rows)
            two = two + dot(p1.astype(BF), rows)
            grad = grad + dot((p0 + p1).astype(BF), ret[a + 1, q * BLK : (q + 1) * BLK, :])
        mixed[m] = (gates[m, 0] * one + gates[m, 1] * two).astype(BF)
        tgrad[m] = grad.astype(BF)

    whole = rgs[...]
    for n in range(7):
        wait(rgr.at[n], rg_r.at[n])
        whole = whole + rgr[n]
    rg[...] = whole

    for arr in range(4):
        wait(snd.at[arr, 0:336, :], a_s.at[arr])
        wait(G.at[arr, :, 0:384], z_s.at[arr])
        wait(G.at[arr, :, 0:1536], x_s.at[arr])
        wait(G.at[arr, :, 0:2048], d_s.at[arr])
        wait(Pt.at[arr, :, 0:1536], rx_s.at[arr])
        wait(Pt.at[arr, :, 0:384], rz_s.at[arr])
        wait(fin.at[arr, 0:336, :], b_s.at[arr])
    for k, half in enumerate((WgH.at[:, 0:HID], WuH.at[:, 0:HID], WdH.at[0:HID, :])):
        wait(half, w_s.at[k])
    for m in range(2):
        for n, buf in enumerate((HC, PG, PU)):
            wait(buf.at[m, :, 0:HID], h_s.at[m, n])
    for k in range(2):
        wait(arR.at[k, 0], ar_s.at[k, 0])
        wait(arR.at[k, 1:4], ar_s.at[k, 1])
        wait(arR.at[k, 4:7], ar_s.at[k, 2])
    wait(gts.at[0:7], gt_s.at[0])
    wait(dts.at[0:7], dt_s.at[0])
    wait(rgr.at[0:7], rg_s.at[0])
    for k, (buf, out) in enumerate(((wg, gg_h), (wu, ug_h), (wd, dg_h))):
        pltpu.make_async_copy(buf, out, o_s.at[k]).wait()


def shards(tokens, expert_ids, router_weight, w_gate, w_up, w_down, cotangent):
    rwt = jnp.pad(router_weight.T, ((0, BLK - 8), (0, 0)))
    big = lambda *dims: pltpu.VMEM(dims, BF)
    wide = lambda *dims: pltpu.VMEM(dims, F32)
    dma = lambda *dims: pltpu.SemaphoreType.DMA(dims)
    vm = pl.BlockSpec(memory_space=pltpu.VMEM)
    anyw = pl.BlockSpec(memory_space=pl.ANY)
    D = 4096
    mixed, tgrad, gg, ug, dg, rg = pl.pallas_call(
        kernel,
        name="expert_layer",
        out_shape=(
            jax.ShapeDtypeStruct((2, BLK, BLK), BF),
            jax.ShapeDtypeStruct((2, BLK, BLK), BF),
            jax.ShapeDtypeStruct((D, HID), BF),
            jax.ShapeDtypeStruct((D, HID), BF),
            jax.ShapeDtypeStruct((HID, D), BF),
            jax.ShapeDtypeStruct((8, BLK), F32),
        ),
        in_specs=[vm, vm, vm, vm, anyw, anyw, anyw],
        out_specs=(vm, vm, anyw, anyw, anyw, vm),
        scratch_shapes=[
            big(4, ROWS, D), big(D, HID), big(D, HID), big(HID, D),
            big(2048, 512), big(2048, 512), big(512, 2048), big(4, ROWS, BLK),
            wide(ROWS, HID), wide(ROWS, HID), wide(ROWS, HID),
            big(2, ROWS, 512), big(2, ROWS, 512), big(2, ROWS, 512), big(2, ROWS, HID),
            wide(2, ROWS, BLK), wide(2, ROWS, BLK),
            big(4, ROWS, 2048), big(4, 4, ROWS, BLK), big(4, 4, ROWS, BLK), big(4, 4, ROWS, BLK),
            big(4, 3, ROWS, BLK), big(4, 3, ROWS, BLK), wide(4, ROWS, BLK), big(4, ROWS, BLK), big(4, ROWS, BLK),
            wide(2, 2, BLK, BLK), wide(2, 2, BLK, BLK), wide(2, BLK, BLK),
            wide(2, 3, 8, BLK), wide(2, 7, 8, BLK), wide(8, 8, BLK), wide(8, 8, BLK), wide(8, 8, BLK), wide(8, 8, BLK),
            wide(8, BLK), wide(7, 8, BLK),
            dma(6), dma(3), dma(3), dma(4), dma(4), dma(4), dma(4, 3), dma(4), dma(4, 4), dma(4, 4), dma(4, 4),
            dma(4), dma(4), dma(2, 3), dma(2, 3),
            dma(4), dma(4, 4), dma(4, 4), dma(4, 4), dma(4), dma(4, 3), dma(4), dma(4),
            dma(2, 3), dma(2, 7), dma(1), dma(1), dma(1), dma(1), dma(1), dma(7), dma(3),
        ],
        compiler_params=pltpu.CompilerParams(
            collective_id=0, has_side_effects=True, vmem_limit_bytes=64 * 1024 * 1024 - 65536 * 2
        ),
    )(tokens, cotangent, expert_ids, rwt, w_gate[0], w_up[0], w_down[0])
    return mixed, tgrad, gg[None], ug[None], dg[None], rg.T


def solution(mesh):
    split = Mesh(mesh.devices.reshape(4, 4, 2, 2, 4), REP + EP)
    in_specs = (
        P(None, EP, REP),
        P(None, EP, None),
        P(REP, None),
        P(EP, None, REP),
        P(EP, None, REP),
        P(EP, REP, None),
        P(None, EP, REP),
    )
    out_specs = (
        P(None, EP, REP),
        P(None, EP, REP),
        P(EP, None, REP),
        P(EP, None, REP),
        P(EP, REP, None),
        P(REP, None),
    )
    return jax.shard_map(shards, mesh=split, in_specs=in_specs, out_specs=out_specs, check_vma=False)
```

```python
import jax
import jax.numpy as jnp
from jax import lax
from jax.experimental import pallas as pl
from jax.experimental.pallas import tpu as pltpu
from jax.sharding import Mesh
from jax.sharding import PartitionSpec as P

MESH = pl.DeviceIdType.MESH
REP = ("zl", "x", "c")
EP = ("zh", "y")
F32 = jnp.float32
BF = jnp.bfloat16
CAP = 48
ROWS = 384
BLK = 128
HID = 256
PEERS = [(dz, dy) for dz in range(2) for dy in range(4) if dz or dy]
HALF = 192
NEAR = (0, 1, 7, 2, 6, 3, 5, 4)


def rem(value, n):
    return lax.rem(value, jnp.int32(n))


def wait(ref, sem):
    pltpu.make_async_copy(ref, ref, sem).wait()


def dot(a, b):
    return jnp.dot(a, b, preferred_element_type=F32)


def dot_tn(a, b):
    return lax.dot_general(a, b, (((0,), (0,)), ((), ())), preferred_element_type=F32)


def dot_nt(a, b):
    return lax.dot_general(a, b, (((1,), (1,)), ((), ())), preferred_element_type=F32)


def iota(rows, lanes, dim):
    return lax.broadcasted_iota(jnp.int32, (rows, lanes), dim).astype(F32)


def to_row(col):
    n = col.shape[0]
    return jnp.sum(jnp.where(iota(n, BLK, 0) == iota(n, BLK, 1), col, 0.0), axis=0, keepdims=True)


def to_col(row, n):
    return jnp.sum(jnp.where(iota(n, BLK, 0) == iota(n, BLK, 1), row, 0.0), axis=1, keepdims=True)


def tile_of(rows):
    sub = iota(8, BLK, 0)
    return jnp.where(sub == 0.0, rows[0], 0.0) + jnp.where(sub == 1.0, rows[1], 0.0)


def sigmoid(v):
    return 1.0 / (1.0 + jnp.exp(-v))


def kernel(
    tok, cot, ids, rwt, wg_h, wu_h, wd_h,
    mixed, tgrad, wg, wu, wd, rg,
    G, WgH, WuH, WdH, snd, HB, XB, AG, AU, HG, HC, PG, PU, HS, gcol, dcol,
    Pt, FX, XL, XR, zs, zr, zo, fin, ret, slots, gates, dmat, arS, arR, gts, gtr, dts, dtr, rgs, rgr,
    w_l, w_s, w_r, a_s, a_r, z_s, z_r, x_s, xl_r, xr_r, f_r, d_s, d_r, h_s, h_r,
    rx_s, rf_r, rl_r, rr_r, rz_s, rz_r, b_s, b_r, ar_s, ar_r, gt_s, gt_r, dt_s, dt_r, rg_s, rg_r, xb_s, xb_r, z3_s, z3_r,
):
    zl = lax.axis_index("zl")
    x = lax.axis_index("x")
    c = lax.axis_index("c")
    zh = lax.axis_index("zh")
    y = lax.axis_index("y")
    right, left, far = rem(x + 1, 4), rem(x + 3, 4), rem(x + 2, 4)
    z = zh * 4 + zl
    e = zh * 4 + y
    oc = 1 - c
    r = zl * 8 + x * 2 + c

    def send(src, dst, ss, rs, dev):
        pltpu.make_async_remote_copy(
            src_ref=src, dst_ref=dst, send_sem=ss, recv_sem=rs, device_id=dev, device_id_type=MESH
        ).start()

    def lanes(index, width=BLK):
        return pl.ds(pl.multiple_of(index * width, width), width)

    def feat(zl_, x_, c_):
        return zl_ * 8 + x_ * 2 + c_

    def col(arr, zl_, x_):
        return G.at[arr, :, lanes(feat(zl_, x_, c))]

    def cap(index):
        return pl.ds(pl.multiple_of(index * CAP, 16), CAP)

    mine = lanes(c, HID)

    barrier = pltpu.get_barrier_semaphore()
    pl.semaphore_signal(barrier, inc=1, device_id={"c": oc}, device_id_type=MESH)
    for j in range(1, 4):
        pl.semaphore_signal(barrier, inc=1, device_id={"x": rem(x + j, 4)}, device_id_type=MESH)
        pl.semaphore_signal(barrier, inc=1, device_id={"zl": rem(zl + j, 4)}, device_id_type=MESH)
    for j in range(1, 4):
        dev = {"zh": 1 - zh, "zl": rem(zl + j, 4)}
        pl.semaphore_signal(barrier, inc=1, device_id=dev, device_id_type=MESH)
    for dz, dy in PEERS:
        dev = {"zh": rem(zh + dz, 2), "y": rem(y + dy, 4)}
        pl.semaphore_signal(barrier, inc=1, device_id=dev, device_id_type=MESH)

    sub, lane = iota(BLK, BLK, 0), iota(BLK, BLK, 1)

    def hits(m):
        both = ids[m].astype(F32)
        first, second = to_col(both[0:1, :], BLK), to_col(both[1:2, :], BLK)
        return first, second, jnp.where(first == lane, 1.0, 0.0), jnp.where(second == lane, 1.0, 0.0)

    def route(m):
        first, second, h0, h1 = hits(m)
        tri = jnp.where(lane < sub, 1.0, 0.0).astype(BF)
        before = dot(tri, (h0 + h1).astype(BF))
        s0 = first * float(CAP) + jnp.sum(h0 * before, axis=1, keepdims=True)
        s1 = second * float(CAP) + jnp.sum(h1 * before, axis=1, keepdims=True)
        slots[m, 0] = jnp.broadcast_to(s0, (BLK, BLK))
        slots[m, 1] = jnp.broadcast_to(s1, (BLK, BLK))
        at = iota(ROWS, BLK, 0)
        match = jnp.where((at == to_row(s0)) | (at == to_row(s1)), 1.0, 0.0).astype(BF)
        for n, rows in enumerate((tok, cot)):
            arr = 2 * m + n
            snd[arr] = dot(match, rows[m]).astype(BF)
            for h in range(2):
                HB[arr, h, cap(y), :] = snd[arr, cap(h * 4 + y), :]

    def logits(m):
        _, _, h0, h1 = hits(m)
        diff = jnp.zeros((BLK, BLK), F32)
        for ex in range(8):
            diff = diff + (h0 - h1)[:, ex : ex + 1] * rwt[ex : ex + 1, :].astype(F32)
        dmat[m] = diff
        return to_row(jnp.sum(tok[m].astype(F32) * diff, axis=1, keepdims=True))

    def y_sends(m):
        for arr in (2 * m, 2 * m + 1):
            for dy in range(1, 4):
                ty = rem(y + dy, 4)
                for h in range(2):
                    send(snd.at[arr, cap(h * 4 + ty), :], HB.at[arr, h, cap(y), :],
                         a_s.at[arr], a_r.at[arr], {"y": ty})

    route(0)
    pl.semaphore_wait(barrier, 17)

    def ar_one(k):
        for j in range(1, 4):
            send(arS.at[k, 0], arR.at[k, j - 1], ar_s.at[k, 0], ar_r.at[k, j - 1], {"zl": rem(zl + j, 4)})

    def ar_two(k):
        total = arS[k, 0]
        for j in range(3):
            wait(arR.at[k, j], ar_r.at[k, j])
            total = total + arR[k, j]
        arS[k, 1] = total
        for j in range(1, 4):
            send(arS.at[k, 1], arR.at[k, 2 + j], ar_s.at[k, 1], ar_r.at[k, 2 + j], {"x": rem(x + j, 4)})

    def ar_three(k):
        total = arS[k, 1]
        for j in range(3, 6):
            wait(arR.at[k, j], ar_r.at[k, j])
            total = total + arR[k, j]
        arS[k, 2] = total
        send(arS.at[k, 2], arR.at[k, 6], ar_s.at[k, 2], ar_r.at[k, 6], {"c": oc})

    def ar_end(k):
        wait(arR.at[k, 6], ar_r.at[k, 6])
        return arS[k, 2] + arR[k, 6]


    y_sends(0)
    arS[0, 0] = tile_of([logits(0), logits(1)])
    ar_one(0)
    route(1)
    y_sends(1)

    pltpu.make_async_copy(wg_h, wg, w_l.at[0]).start()
    pltpu.make_async_copy(wu_h, wu, w_l.at[1]).start()
    pltpu.make_async_copy(wd_h, wd, w_l.at[2]).start()

    @pl.loop(0, 16)
    def _(b):
        at = feat(b // 4, b % 4, c)
        pltpu.make_async_copy(wg_h.at[lanes(at), :], WgH.at[lanes(b), mine], w_l.at[3]).start()
        pltpu.make_async_copy(wu_h.at[lanes(at), :], WuH.at[lanes(b), mine], w_l.at[4]).start()
        pltpu.make_async_copy(wd_h.at[:, lanes(at)], WdH.at[mine, lanes(b)], w_l.at[5]).start()

    @pl.loop(0, 16)
    def _(b):
        at = feat(b // 4, b % 4, oc)
        send(wg_h.at[lanes(at), :], WgH.at[lanes(b), mine], w_s.at[0], w_r.at[0], {"c": oc})
        send(wu_h.at[lanes(at), :], WuH.at[lanes(b), mine], w_s.at[1], w_r.at[1], {"c": oc})
        send(wd_h.at[:, lanes(at)], WdH.at[mine, lanes(b)], w_s.at[2], w_r.at[2], {"c": oc})

    def place(arr, z8, x_):
        return G.at[arr, pl.ds(pl.multiple_of(z8 // 4 * HALF, HALF), HALF), lanes(feat(rem(z8, 4), x_, c))]

    def spread_block(arr, z8, j):
        here = place(arr, z8, x)
        send(here, here, x_s.at[arr], xl_r.at[arr, j], {"x": right})
        send(here, here, x_s.at[arr], xr_r.at[arr, j], {"x": left})
        send(here, here, d_s.at[arr], d_r.at[arr], {"c": oc})

    def at_z(z8):
        return {"zh": z8 // 4, "zl": rem(z8, 4)}

    def stage_a(arr):
        wait(snd.at[arr, 0:288, :], a_r.at[arr])
        here = place(arr, z, x)
        for j in range(1, 8):
            to = rem(z + 8 - NEAR[j], 8)
            send(HB.at[arr, to // 4], here, z_s.at[arr], z_r.at[arr, j], at_z(to))
        here[...] = HB[arr, zh]
        spread_block(arr, z, 0)

    def stage_b(arr):
        for j in range(1, 8):
            zj = rem(z + NEAR[j], 8)
            wait(place(arr, zj, x), z_r.at[arr, j])
            spread_block(arr, zj, j)

    def stage_c(arr):
        for j in range(8):
            zj = rem(z + NEAR[j], 8)
            here = place(arr, zj, left)
            wait(here, xl_r.at[arr, j])
            if j % 2 == 0:
                send(here, here, x_s.at[arr], f_r.at[arr, j], {"x": right})
            send(here, here, d_s.at[arr], d_r.at[arr], {"c": oc})
            here = place(arr, zj, right)
            wait(here, xr_r.at[arr, j])
            if j % 2 == 1:
                send(here, here, x_s.at[arr], f_r.at[arr, j], {"x": left})
            send(here, here, d_s.at[arr], d_r.at[arr], {"c": oc})

    def b_start():
        wait(snd.at[3, 0:288, :], a_r.at[3])
        send(HB.at[3], XB.at[0], xb_s.at[0], xb_r.at[0], {"x": right})
        send(HB.at[3], XB.at[1], xb_s.at[0], xb_r.at[1], {"x": left})

    def b_forward():
        wait(XB.at[0], xb_r.at[0])
        send(XB.at[0, 0], XB.at[2, 0], xb_s.at[0], xb_r.at[2], {"x": right})
        wait(XB.at[1], xb_r.at[1])
        send(XB.at[1, 1], XB.at[2, 1], xb_s.at[0], xb_r.at[3], {"x": left})

    def b_out(q, src, x_):
        here = place(3, z, x_)
        for j in range(1, 8):
            to = rem(z + 8 - NEAR[j], 8)
            send(src.at[to // 4], here, z3_s.at[0], z3_r.at[q, j], at_z(to))
        here[...] = src[zh]
        send(here, here, d_s.at[3], d_r.at[3], {"c": oc})

    def b_spread():
        b_out(0, HB.at[3], x)
        b_out(1, XB.at[0], left)
        b_out(2, XB.at[1], right)
        wait(XB.at[2, 0], xb_r.at[2])
        wait(XB.at[2, 1], xb_r.at[3])
        b_out(3, XB.at[2], far)

    def b_take(q):
        for j in range(1, 8):
            here = place(3, rem(z + NEAR[j], 8), (x, left, right, far)[q])
            wait(here, z3_r.at[q, j])
            send(here, here, d_s.at[3], d_r.at[3], {"c": oc})

    def stage_d(arr):
        for j in range(8):
            here = place(arr, rem(z + NEAR[j], 8), far)
            wait(here, f_r.at[arr, j])
            send(here, here, d_s.at[arr], d_r.at[arr], {"c": oc})

    def stage_e(arr):
        wait(G.at[arr, :, 0:2048], d_r.at[arr])

    def make_gates():
        total = ar_end(0)
        for m in range(2):
            diff = to_col(total[m : m + 1, :], BLK)
            gates[m, 0] = jnp.broadcast_to(sigmoid(diff), (BLK, BLK))
            gates[m, 1] = jnp.broadcast_to(sigmoid(-diff), (BLK, BLK))

        @pl.loop(0, 8)
        def _(ex):
            at = lane + (ex * CAP).astype(F32)
            rows = []
            for m in range(2):
                picked = jnp.where(slots[m, 0] == at, gates[m, 0], 0.0)
                picked = picked + jnp.where(slots[m, 1] == at, gates[m, 1], 0.0)
                rows.append(jnp.sum(picked, axis=0, keepdims=True))
            gts[ex] = tile_of(rows)

        gtr[e] = gts[e]
        for n, (dz, dy) in enumerate(PEERS):
            tz, ty = rem(zh + dz, 2), rem(y + dy, 4)
            send(gts.at[tz * 4 + ty], gtr.at[e], gt_s.at[0], gt_r.at[0], {"zh": tz, "y": ty})

    def take_gates():
        wait(gts.at[0:7], gt_r.at[0])

        @pl.loop(0, 8)
        def _(s):
            tile = gtr[s]
            for m in range(2):
                gcol[m, cap(s), :] = jnp.broadcast_to(to_col(tile[m : m + 1, :], CAP), (CAP, BLK))

    def pre(m):
        AG[...] = jnp.zeros_like(AG)
        AU[...] = jnp.zeros_like(AU)

        @pl.loop(0, 4)
        def _(k):
            rows = G[2 * m, :, lanes(k, 1024)]
            AG[...] += dot(rows, wg[lanes(k, 1024), :])
            AU[...] += dot(rows, wu[lanes(k, 1024), :])

    def back(m):
        HG[...] = jnp.zeros_like(HG)

        @pl.loop(0, 4)
        def _(k):
            HG[...] += dot_nt(G[2 * m + 1, :, lanes(k, 1024)], wd[:, lanes(k, 1024)])

        @pl.loop(0, 6)
        def _(i):
            rows = lanes(i, 64)
            pg, pu, hr = AG[rows, :], AU[rows, :], HG[rows, :]
            g = gcol[m, rows, 0:1]
            sig = sigmoid(pg)
            act = pg * sig
            hb = (act * pu).astype(BF)
            hw = hb.astype(F32)
            dcol[m, rows, :] = jnp.broadcast_to(jnp.sum(hw * hr, axis=1, keepdims=True), (64, BLK))
            hs = hr * g
            HC[m, rows, mine] = hb
            PG[m, rows, mine] = (hs * pu * (sig * (1.0 + pg * (1.0 - sig)))).astype(BF)
            PU[m, rows, mine] = (hs * act).astype(BF)
            HS[m, rows, :] = (hw * g).astype(BF)

        for n, buf in enumerate((HC, PG, PU)):
            send(buf.at[m, :, mine], buf.at[m, :, mine], h_s.at[m, n], h_r.at[m, n], {"c": oc})

    def part(a, zl_, x_):
        return Pt.at[a, :, lanes(zl_ * 4 + x_)]

    def far_sends(a):
        for zp in range(4):
            to = right if zp % 2 == 0 else left
            send(part(a, zp, far), FX.at[a, zp], rx_s.at[a], rf_r.at[a, zp], {"x": to})

    def near_sends(a):
        for zp in range(4):
            if zp % 2 == 0:
                send(part(a, zp, left), XR.at[a, zp], rx_s.at[a], rr_r.at[a, zp], {"x": left})
            else:
                send(part(a, zp, right), XL.at[a, zp], rx_s.at[a], rl_r.at[a, zp], {"x": right})

    def outs(m):
        wait(HC.at[m, :, 0:HID], h_r.at[m, 0])

        @pl.loop(0, 4)
        def _(q):
            Pt[2 * m, :, lanes(q, 512)] = dot(HC[m], WdH[:, lanes(q, 512)]).astype(BF)

    def ins(m):
        wait(PG.at[m, :, 0:HID], h_r.at[m, 1])
        wait(PU.at[m, :, 0:HID], h_r.at[m, 2])

        @pl.loop(0, 4)
        def _(q):
            at = lanes(q, 512)
            Pt[2 * m + 1, :, at] = (dot_nt(PG[m], WgH[at, :]) + dot_nt(PU[m], WuH[at, :])).astype(BF)

    def second_sends(a):
        for zp in range(4):
            wait(FX.at[a, zp], rf_r.at[a, zp])
            tx = right if zp % 2 == 0 else left
            where = lanes(zp * 4 + tx)
            Pt[a, :, where] = (Pt[a, :, where].astype(F32) + FX[a, zp].astype(F32)).astype(BF)
            if zp % 2 == 0:
                send(part(a, zp, tx), XL.at[a, zp], rx_s.at[a], rl_r.at[a, zp], {"x": right})
            else:
                send(part(a, zp, tx), XR.at[a, zp], rx_s.at[a], rr_r.at[a, zp], {"x": left})

    def third_sends(a, zps=(0, 1, 2, 3)):
        for zp in zps:
            wait(XL.at[a, zp], rl_r.at[a, zp])
            wait(XR.at[a, zp], rr_r.at[a, zp])
            total = Pt[a, :, lanes(zp * 4 + x)].astype(F32)
            total = total + XL[a, zp].astype(F32) + XR[a, zp].astype(F32)
            for h in range(2):
                to = h * 4 + zp
                step = rem(z + 8 - to, 8)
                rows = total[h * HALF : (h + 1) * HALF, :]
                zs[a, to] = rows.astype(BF)

                @pl.when(z == to)
                def _():
                    zo[a, zh] = rows
                    zo[a, 1 - zh] = jnp.zeros((HALF, BLK), F32)

                @pl.when(z != to)
                def _():
                    send(zs.at[a, to], zr.at[a, step - 1], rz_s.at[a], rz_r.at[a, step - 1], {"zh": h, "zl": zp})

    def finish(a):
        for j in range(1, 8):
            step = NEAR[j]
            h = rem(z + step, 8) // 4
            wait(zr.at[a, step - 1], rz_r.at[a, step - 1])
            zo[a, h] += zr[a, step - 1].astype(F32)
        for h in range(2):
            fin[a, h] = zo[a, h].astype(BF)
            ret[a, cap(h * 4 + y), :] = fin[a, h, cap(y), :]
        for dy in range(1, 4):
            ty = rem(y + dy, 4)
            for h in range(2):
                send(fin.at[a, h, cap(ty), :], ret.at[a, cap(h * 4 + y), :], b_s.at[a], b_r.at[a], {"y": ty})

    def send_dots():
        @pl.loop(0, 8)
        def _(s):
            dts[s] = tile_of([to_row(dcol[m, cap(s), :]) for m in range(2)])

        dtr[e] = dts[e]
        for dz, dy in PEERS:
            tz, ty = rem(zh + dz, 2), rem(y + dy, 4)
            send(dts.at[tz * 4 + ty], dtr.at[e], dt_s.at[0], dt_r.at[0], {"zh": tz, "y": ty})

    def take_dots():
        wait(dts.at[0:7], dt_r.at[0])
        rows = []
        for m in range(2):
            total = jnp.zeros((BLK, BLK), F32)
            for ex in range(8):
                at = lane + float(ex * CAP)
                row = dtr[ex][m : m + 1, :]
                total = total + jnp.where(slots[m, 0] == at, row, 0.0) - jnp.where(slots[m, 1] == at, row, 0.0)
            rows.append(to_row(jnp.sum(total, axis=1, keepdims=True)))
        arS[1, 0] = tile_of(rows)
        ar_one(1)

    def weight_grads(lo, hi):
        @pl.loop(lo, hi)
        def _(i):
            at = lanes(i, 512)
            t0, t1 = G[0, :, at], G[2, :, at]
            wg[at, :] = (dot_tn(t0, PG[0, :, mine]) + dot_tn(t1, PG[1, :, mine])).astype(BF)
            wu[at, :] = (dot_tn(t0, PU[0, :, mine]) + dot_tn(t1, PU[1, :, mine])).astype(BF)
            wd[:, at] = (dot_tn(HS[0], G[1, :, at]) + dot_tn(HS[1], G[3, :, at])).astype(BF)

    stage_a(0)
    stage_a(1)
    b_start()
    stage_a(2)
    ar_two(0)
    b_forward()
    ar_three(0)
    make_gates()
    b_spread()
    stage_b(0)
    stage_c(0)
    stage_b(1)
    stage_d(0)
    stage_c(1)
    stage_b(2)
    stage_e(0)
    for k, buf in enumerate((wg, wu, wd)):
        pltpu.make_async_copy(buf, buf, w_l.at[k]).wait()
    for k, half in enumerate((WgH.at[:, 0:HID], WuH.at[:, 0:HID], WdH.at[0:HID, :])):
        wait(half, w_l.at[3 + k])
        wait(half, w_r.at[k])
    pre(0)
    stage_d(1)
    stage_c(2)
    stage_e(1)
    take_gates()
    back(0)
    outs(0)
    far_sends(0)
    near_sends(0)
    ins(0)
    stage_d(2)
    far_sends(1)
    second_sends(0)
    near_sends(1)
    b_take(0)
    stage_e(2)
    pre(1)
    b_take(1)
    second_sends(1)
    b_take(2)
    b_take(3)
    stage_e(3)
    back(1)
    outs(1)
    far_sends(2)
    near_sends(2)
    send_dots()
    ins(1)
    far_sends(3)
    second_sends(2)
    near_sends(3)
    third_sends(0)
    third_sends(1)
    weight_grads(0, 3)
    take_dots()
    third_sends(2, (0, 1))
    second_sends(3)
    third_sends(2, (2, 3))
    weight_grads(3, 5)
    finish(0)
    ar_two(1)
    finish(1)
    third_sends(3, (0, 1))
    weight_grads(5, 7)
    ar_three(1)
    third_sends(3, (2, 3))
    weight_grads(7, 8)

    total = ar_end(1)
    share = jnp.zeros((BLK, BLK), F32)
    deltas = []
    for m in range(2):
        _, _, h0, h1 = hits(m)
        delta = to_col(total[m : m + 1, :], BLK) * gates[m, 0] * gates[m, 1]
        deltas.append(delta)
        share = share + lax.dot_general(
            delta * (h0 - h1), tok[m].astype(F32), (((0,), (0,)), ((), ())),
            preferred_element_type=F32, precision=lax.Precision.HIGHEST,
        )
    rgs[...] = share[0:8, :]
    for n, (dz, dy) in enumerate(PEERS):
        tz, ty = rem(zh + dz, 2), rem(y + dy, 4)
        send(rgs, rgr.at[n], rg_s.at[0], rg_r.at[n], {"zh": tz, "y": ty})
    finish(2)
    finish(3)

    for m in range(2):
        a = 2 * m
        wait(ret.at[a, 0:288, :], b_r.at[a])
        wait(ret.at[a + 1, 0:288, :], b_r.at[a + 1])
        one = jnp.zeros((BLK, BLK), F32)
        two = jnp.zeros((BLK, BLK), F32)
        grad = deltas[m] * dmat[m]
        for q in range(3):
            at = lane + float(q * BLK)
            p0 = jnp.where(slots[m, 0] == at, 1.0, 0.0)
            p1 = jnp.where(slots[m, 1] == at, 1.0, 0.0)
            rows = ret[a, q * BLK : (q + 1) * BLK, :]
            one = one + dot(p0.astype(BF), rows)
            two = two + dot(p1.astype(BF), rows)
            grad = grad + dot((p0 + p1).astype(BF), ret[a + 1, q * BLK : (q + 1) * BLK, :])
        mixed[m] = (gates[m, 0] * one + gates[m, 1] * two).astype(BF)
        tgrad[m] = grad.astype(BF)

    whole = rgs[...]
    for n in range(7):
        wait(rgr.at[n], rg_r.at[n])
        whole = whole + rgr[n]
    rg[...] = whole

    for arr in range(4):
        wait(snd.at[arr, 0:288, :], a_s.at[arr])
        if arr < 3:
            wait(G.at[arr, 0:HALF, 0:896], z_s.at[arr])
            wait(G.at[arr, :, 0:1536], x_s.at[arr])
        wait(G.at[arr, :, 0:2048], d_s.at[arr])
        wait(Pt.at[arr, :, 0:1536], rx_s.at[arr])
        wait(zr.at[arr], rz_s.at[arr])
        wait(ret.at[arr, 0:288, :], b_s.at[arr])
    wait(zr.at[0, 0:6], xb_s.at[0])
    wait(G.at[3, 0:HALF, 0:3584], z3_s.at[0])
    for k, half in enumerate((WgH.at[:, 0:HID], WuH.at[:, 0:HID], WdH.at[0:HID, :])):
        wait(half, w_s.at[k])
    for m in range(2):
        for n, buf in enumerate((HC, PG, PU)):
            wait(buf.at[m, :, 0:HID], h_s.at[m, n])
    for k in range(2):
        wait(arR.at[k, 0:3], ar_s.at[k, 0])
        wait(arR.at[k, 3:6], ar_s.at[k, 1])
        wait(arR.at[k, 6], ar_s.at[k, 2])
    wait(gts.at[0:7], gt_s.at[0])
    wait(dts.at[0:7], dt_s.at[0])
    wait(rgr.at[0:7], rg_s.at[0])


def write_out(*refs):
    sems = refs[12]
    copies = [pltpu.make_async_copy(refs[k], refs[6 + k], sems.at[k]) for k in range(6)]
    for copy in copies:
        copy.start()
    for copy in copies:
        copy.wait()


def shards(tokens, expert_ids, router_weight, w_gate, w_up, w_down, cotangent):
    big = lambda *dims: pltpu.VMEM(dims, BF)
    wide = lambda *dims: pltpu.VMEM(dims, F32)
    dma = lambda *dims: pltpu.SemaphoreType.DMA(dims)
    vm = pl.BlockSpec(memory_space=pltpu.VMEM)
    anyw = pl.BlockSpec(memory_space=pl.ANY)
    D = 4096
    results = pl.pallas_call(
        kernel,
        name="expert_layer",
        out_shape=(
            big(2, BLK, BLK), big(2, BLK, BLK), big(D, HID), big(D, HID), big(HID, D), wide(8, BLK),
        ),
        in_specs=[vm, vm, vm, vm, anyw, anyw, anyw],
        out_specs=(vm,) * 6,
        scratch_shapes=[
            big(4, ROWS, D),
            big(2048, 512), big(2048, 512), big(512, 2048), big(4, ROWS, BLK), big(4, 2, HALF, BLK), big(3, 2, HALF, BLK),
            wide(ROWS, HID), wide(ROWS, HID), wide(ROWS, HID),
            big(2, ROWS, 512), big(2, ROWS, 512), big(2, ROWS, 512), big(2, ROWS, HID),
            wide(2, ROWS, BLK), wide(2, ROWS, BLK),
            big(4, ROWS, 2048), big(4, 4, ROWS, BLK), big(4, 4, ROWS, BLK), big(4, 4, ROWS, BLK),
            big(4, 8, HALF, BLK), big(4, 7, HALF, BLK), wide(4, 2, HALF, BLK), big(4, 2, HALF, BLK), big(4, ROWS, BLK),
            wide(2, 2, BLK, BLK), wide(2, 2, BLK, BLK), wide(2, BLK, BLK),
            wide(2, 3, 8, BLK), wide(2, 7, 8, BLK), wide(8, 8, BLK), wide(8, 8, BLK), wide(8, 8, BLK), wide(8, 8, BLK),
            wide(8, BLK), wide(7, 8, BLK),
            dma(6), dma(3), dma(3), dma(4), dma(4), dma(4), dma(3, 8), dma(4), dma(3, 8), dma(3, 8), dma(3, 8),
            dma(4), dma(4), dma(2, 3), dma(2, 3),
            dma(4), dma(4, 4), dma(4, 4), dma(4, 4), dma(4), dma(4, 7), dma(4), dma(4),
            dma(2, 3), dma(2, 7), dma(1), dma(1), dma(1), dma(1), dma(1), dma(7), dma(1), dma(4), dma(1), dma(4, 8),
        ],
        compiler_params=pltpu.CompilerParams(
            collective_id=0, has_side_effects=True, vmem_limit_bytes=52 * 1024 * 1024
        ),
    )(tokens, cotangent, expert_ids.transpose(0, 2, 1), router_weight.T, w_gate[0], w_up[0], w_down[0])
    mixed, tgrad, gg, ug, dg, rg = pl.pallas_call(
        write_out,
        name="write_out",
        out_shape=tuple(jax.ShapeDtypeStruct(v.shape, v.dtype) for v in results),
        in_specs=[vm] * 6,
        out_specs=(anyw,) * 6,
        scratch_shapes=[dma(6)],
        compiler_params=pltpu.CompilerParams(vmem_limit_bytes=1024 * 1024),
    )(*(pltpu.with_memory_space_constraint(v, pltpu.VMEM) for v in results))
    return mixed, tgrad, gg[None], ug[None], dg[None], rg.T


def solution(mesh):
    split = Mesh(mesh.devices.reshape(4, 4, 2, 2, 4), REP + EP)
    in_specs = (
        P(None, EP, REP),
        P(None, EP, None),
        P(REP, None),
        P(EP, None, REP),
        P(EP, None, REP),
        P(EP, REP, None),
        P(None, EP, REP),
    )
    out_specs = (
        P(None, EP, REP),
        P(None, EP, REP),
        P(EP, None, REP),
        P(EP, None, REP),
        P(EP, REP, None),
        P(REP, None),
    )
    return jax.shard_map(shards, mesh=split, in_specs=in_specs, out_specs=out_specs, check_vma=False)
```

```python
import jax
import jax.numpy as jnp
from jax import lax
from jax.experimental import pallas as pl
from jax.experimental.pallas import tpu as pltpu
from jax.sharding import Mesh
from jax.sharding import PartitionSpec as P

MESH = pl.DeviceIdType.MESH
REP = ("zl", "x", "c")
EP = ("zh", "y")
F32 = jnp.float32
BF = jnp.bfloat16
CAP = 48
ROWS = 384
BLK = 128
HID = 256
PEERS = [(dz, dy) for dz in range(2) for dy in range(4) if dz or dy]
HALF = 192
TURN = (0, 1, 3, 2)
NEAR = (0, 1, 7, 2, 6, 3, 5, 4)


def rem(value, n):
    return lax.rem(value, jnp.int32(n))


def wait(ref, sem):
    pltpu.make_async_copy(ref, ref, sem).wait()


def dot(a, b):
    return jnp.dot(a, b, preferred_element_type=F32)


def dot_tn(a, b):
    return lax.dot_general(a, b, (((0,), (0,)), ((), ())), preferred_element_type=F32)


def dot_nt(a, b):
    return lax.dot_general(a, b, (((1,), (1,)), ((), ())), preferred_element_type=F32)


def iota(rows, lanes, dim):
    return lax.broadcasted_iota(jnp.int32, (rows, lanes), dim).astype(F32)


def to_row(col):
    n = col.shape[0]
    return jnp.sum(jnp.where(iota(n, BLK, 0) == iota(n, BLK, 1), col, 0.0), axis=0, keepdims=True)


def to_col(row, n):
    return jnp.sum(jnp.where(iota(n, BLK, 0) == iota(n, BLK, 1), row, 0.0), axis=1, keepdims=True)


def tile_of(rows):
    sub = iota(8, BLK, 0)
    return jnp.where(sub == 0.0, rows[0], 0.0) + jnp.where(sub == 1.0, rows[1], 0.0)


def sigmoid(v):
    return 1.0 / (1.0 + jnp.exp(-v))


def kernel(
    tok, cot, ids, rwt, wg_h, wu_h, wd_h,
    mixed, tgrad, wg, wu, wd, rg,
    G, WgH, WuH, WdH, snd, HB, XB, AG, AU, HG, HC, PG, PU, HS, gcol, dcol,
    Pt, FX, XL, XR, zs, zr, zo, fin, ret, slots, gates, dmat, arS, arR, gts, gtr, dts, dtr, rgs, rgr,
    w_l, w_s, w_r, a_s, a_r, z_s, z_r, x_s, xl_r, xr_r, f_r, d_s, d_r, h_s, h_r,
    rx_s, rf_r, rl_r, rr_r, rz_s, rz_r, b_s, b_r, ar_s, ar_r, gt_s, gt_r, dt_s, dt_r, rg_s, rg_r, xb_s, xb_r, z3_s, z3_r,
):
    zl = lax.axis_index("zl")
    x = lax.axis_index("x")
    c = lax.axis_index("c")
    zh = lax.axis_index("zh")
    y = lax.axis_index("y")
    right, left, far = rem(x + 1, 4), rem(x + 3, 4), rem(x + 2, 4)
    z = zh * 4 + zl
    e = zh * 4 + y
    oc = 1 - c
    r = zl * 8 + x * 2 + c

    def send(src, dst, ss, rs, dev):
        pltpu.make_async_remote_copy(
            src_ref=src, dst_ref=dst, send_sem=ss, recv_sem=rs, device_id=dev, device_id_type=MESH
        ).start()

    def lanes(index, width=BLK):
        return pl.ds(pl.multiple_of(index * width, width), width)

    def feat(zl_, x_, c_):
        return zl_ * 8 + x_ * 2 + c_

    def col(arr, zl_, x_):
        return G.at[arr, :, lanes(feat(zl_, x_, c))]

    def cap(index):
        return pl.ds(pl.multiple_of(index * CAP, 16), CAP)

    mine = lanes(c, HID)

    barrier = pltpu.get_barrier_semaphore()
    pl.semaphore_signal(barrier, inc=1, device_id={"c": oc}, device_id_type=MESH)
    for j in range(1, 4):
        pl.semaphore_signal(barrier, inc=1, device_id={"x": rem(x + j, 4)}, device_id_type=MESH)
        pl.semaphore_signal(barrier, inc=1, device_id={"zl": rem(zl + j, 4)}, device_id_type=MESH)
    for j in range(1, 4):
        dev = {"zh": 1 - zh, "zl": rem(zl + j, 4)}
        pl.semaphore_signal(barrier, inc=1, device_id=dev, device_id_type=MESH)
    for dz, dy in PEERS:
        dev = {"zh": rem(zh + dz, 2), "y": rem(y + dy, 4)}
        pl.semaphore_signal(barrier, inc=1, device_id=dev, device_id_type=MESH)

    sub, lane = iota(BLK, BLK, 0), iota(BLK, BLK, 1)

    def hits(m):
        both = ids[m].astype(F32)
        first, second = to_col(both[0:1, :], BLK), to_col(both[1:2, :], BLK)
        return first, second, jnp.where(first == lane, 1.0, 0.0), jnp.where(second == lane, 1.0, 0.0)

    def route(m):
        first, second, h0, h1 = hits(m)
        tri = jnp.where(lane < sub, 1.0, 0.0).astype(BF)
        before = dot(tri, (h0 + h1).astype(BF))
        s0 = first * float(CAP) + jnp.sum(h0 * before, axis=1, keepdims=True)
        s1 = second * float(CAP) + jnp.sum(h1 * before, axis=1, keepdims=True)
        slots[m, 0] = jnp.broadcast_to(s0, (BLK, BLK))
        slots[m, 1] = jnp.broadcast_to(s1, (BLK, BLK))
        at = iota(ROWS, BLK, 0)
        match = jnp.where((at == to_row(s0)) | (at == to_row(s1)), 1.0, 0.0).astype(BF)
        for n, rows in enumerate((tok, cot)):
            arr = 2 * m + n
            snd[arr] = dot(match, rows[m]).astype(BF)
            for h in range(2):
                HB[arr, h, cap(y), :] = snd[arr, cap(h * 4 + y), :]

    def logits(m):
        _, _, h0, h1 = hits(m)
        diff = jnp.zeros((BLK, BLK), F32)
        for ex in range(8):
            diff = diff + (h0 - h1)[:, ex : ex + 1] * rwt[ex : ex + 1, :].astype(F32)
        dmat[m] = diff
        return to_row(jnp.sum(tok[m].astype(F32) * diff, axis=1, keepdims=True))

    def y_sends(m):
        for arr in (2 * m, 2 * m + 1):
            for dy in range(1, 4):
                ty = rem(y + dy, 4)
                for h in range(2):
                    send(snd.at[arr, cap(h * 4 + ty), :], HB.at[arr, h, cap(y), :],
                         a_s.at[0], a_r.at[arr], {"y": ty})

    route(0)
    pl.semaphore_wait(barrier, 17)

    def ar_one(k):
        for j in range(1, 4):
            send(arS.at[k, 0], arR.at[k, j - 1], ar_s.at[0], ar_r.at[k, 0], {"zl": rem(zl + j, 4)})

    def ar_two(k):
        total = arS[k, 0]
        wait(arR.at[k, 0:3], ar_r.at[k, 0])
        for j in range(3):
            total = total + arR[k, j]
        arS[k, 1] = total
        for j in range(1, 4):
            send(arS.at[k, 1], arR.at[k, 2 + j], ar_s.at[0], ar_r.at[k, 1], {"x": rem(x + j, 4)})

    def ar_three(k):
        total = arS[k, 1]
        wait(arR.at[k, 3:6], ar_r.at[k, 1])
        for j in range(3, 6):
            total = total + arR[k, j]
        arS[k, 2] = total
        send(arS.at[k, 2], arR.at[k, 6], ar_s.at[0], ar_r.at[k, 2], {"c": oc})

    def ar_end(k):
        wait(arR.at[k, 6], ar_r.at[k, 2])
        return arS[k, 2] + arR[k, 6]


    y_sends(0)
    arS[0, 0] = tile_of([logits(0), logits(1)])
    ar_one(0)
    route(1)
    y_sends(1)

    pltpu.make_async_copy(wg_h, wg, w_l.at[0]).start()
    pltpu.make_async_copy(wu_h, wu, w_l.at[1]).start()
    pltpu.make_async_copy(wd_h, wd, w_l.at[2]).start()

    @pl.loop(0, 16)
    def _(b):
        at = feat(b // 4, b % 4, c)
        pltpu.make_async_copy(wg_h.at[lanes(at), :], WgH.at[lanes(b), mine], w_l.at[3]).start()
        pltpu.make_async_copy(wu_h.at[lanes(at), :], WuH.at[lanes(b), mine], w_l.at[4]).start()
        pltpu.make_async_copy(wd_h.at[:, lanes(at)], WdH.at[mine, lanes(b)], w_l.at[5]).start()

    @pl.loop(0, 16)
    def _(b):
        at = feat(b // 4, b % 4, oc)
        send(wg_h.at[lanes(at), :], WgH.at[lanes(b), mine], w_s.at[0], w_r.at[0], {"c": oc})
        send(wu_h.at[lanes(at), :], WuH.at[lanes(b), mine], w_s.at[1], w_r.at[1], {"c": oc})
        send(wd_h.at[:, lanes(at)], WdH.at[mine, lanes(b)], w_s.at[2], w_r.at[2], {"c": oc})

    def place(arr, z8, x_):
        return G.at[arr, pl.ds(pl.multiple_of(z8 // 4 * HALF, HALF), HALF), lanes(feat(rem(z8, 4), x_, c))]

    def spread_block(arr, z8, j):
        here = place(arr, z8, x)
        send(here, here, x_s.at[0], xl_r.at[arr, j], {"x": right})
        send(here, here, x_s.at[0], xr_r.at[arr, j], {"x": left})
        send(here, here, d_s.at[0], d_r.at[arr], {"c": oc})

    def at_z(z8):
        return {"zh": z8 // 4, "zl": rem(z8, 4)}

    def stage_a(arr):
        wait(snd.at[arr, 0:288, :], a_r.at[arr])
        here = place(arr, z, x)
        for j in range(1, 8):
            to = rem(z + 8 - NEAR[j], 8)
            send(HB.at[arr, to // 4], here, z_s.at[0], z_r.at[arr, j], at_z(to))
        here[...] = HB[arr, zh]
        spread_block(arr, z, 0)

    def stage_b(arr):
        for j in range(1, 8):
            zj = rem(z + NEAR[j], 8)
            wait(place(arr, zj, x), z_r.at[arr, j])
            spread_block(arr, zj, j)

    def stage_c(arr):
        for j in range(8):
            zj = rem(z + NEAR[j], 8)
            here = place(arr, zj, left)
            wait(here, xl_r.at[arr, j])
            if j % 2 == 0:
                send(here, here, x_s.at[0], f_r.at[arr, j], {"x": right})
            send(here, here, d_s.at[0], d_r.at[arr], {"c": oc})
            here = place(arr, zj, right)
            wait(here, xr_r.at[arr, j])
            if j % 2 == 1:
                send(here, here, x_s.at[0], f_r.at[arr, j], {"x": left})
            send(here, here, d_s.at[0], d_r.at[arr], {"c": oc})

    def b_start():
        wait(snd.at[3, 0:288, :], a_r.at[3])
        send(HB.at[3], XB.at[0], xb_s.at[0], xb_r.at[0], {"x": right})
        send(HB.at[3], XB.at[1], xb_s.at[0], xb_r.at[1], {"x": left})

    def b_forward():
        wait(XB.at[0], xb_r.at[0])
        send(XB.at[0, 0], XB.at[2, 0], xb_s.at[0], xb_r.at[2], {"x": right})
        wait(XB.at[1], xb_r.at[1])
        send(XB.at[1, 1], XB.at[2, 1], xb_s.at[0], xb_r.at[3], {"x": left})

    def b_out(q, src, x_):
        here = place(3, z, x_)
        for j in range(1, 8):
            to = rem(z + 8 - NEAR[j], 8)
            send(src.at[to // 4], here, z3_s.at[0], z3_r.at[q], at_z(to))
        here[...] = src[zh]
        send(here, here, d_s.at[0], d_r.at[3], {"c": oc})

    def b_spread():
        b_out(0, HB.at[3], x)
        b_out(1, XB.at[0], left)
        b_out(2, XB.at[1], right)
        wait(XB.at[2, 0], xb_r.at[2])
        wait(XB.at[2, 1], xb_r.at[3])
        b_out(3, XB.at[2], far)

    def b_take(q):
        wait(zr.at[0], z3_r.at[q])
        for j in range(1, 8):
            here = place(3, rem(z + NEAR[j], 8), (x, left, right, far)[q])
            send(here, here, d_s.at[0], d_r.at[3], {"c": oc})

    def stage_d(arr):
        for j in range(8):
            here = place(arr, rem(z + NEAR[j], 8), far)
            wait(here, f_r.at[arr, j])
            send(here, here, d_s.at[0], d_r.at[arr], {"c": oc})

    def stage_e(arr):
        wait(G.at[arr, :, 0:2048], d_r.at[arr])

    def make_gates():
        total = ar_end(0)
        for m in range(2):
            diff = to_col(total[m : m + 1, :], BLK)
            gates[m, 0] = jnp.broadcast_to(sigmoid(diff), (BLK, BLK))
            gates[m, 1] = jnp.broadcast_to(sigmoid(-diff), (BLK, BLK))

        @pl.loop(0, 8)
        def _(ex):
            at = lane + (ex * CAP).astype(F32)
            rows = []
            for m in range(2):
                picked = jnp.where(slots[m, 0] == at, gates[m, 0], 0.0)
                picked = picked + jnp.where(slots[m, 1] == at, gates[m, 1], 0.0)
                rows.append(jnp.sum(picked, axis=0, keepdims=True))
            gts[ex] = tile_of(rows)

        gtr[e] = gts[e]
        for n, (dz, dy) in enumerate(PEERS):
            tz, ty = rem(zh + dz, 2), rem(y + dy, 4)
            send(gts.at[tz * 4 + ty], gtr.at[e], gt_s.at[0], gt_r.at[0], {"zh": tz, "y": ty})

    def take_gates():
        wait(gts.at[0:7], gt_r.at[0])

        @pl.loop(0, 8)
        def _(s):
            tile = gtr[s]
            for m in range(2):
                gcol[m, cap(s), :] = jnp.broadcast_to(to_col(tile[m : m + 1, :], CAP), (CAP, BLK))

    def pre(m):
        AG[...] = jnp.zeros_like(AG)
        AU[...] = jnp.zeros_like(AU)

        @pl.loop(0, 4)
        def _(k):
            rows = G[2 * m, :, lanes(k, 1024)]
            AG[...] += dot(rows, wg[lanes(k, 1024), :])
            AU[...] += dot(rows, wu[lanes(k, 1024), :])

    def hid(m):
        @pl.loop(0, 6)
        def _(i):
            rows = lanes(i, 64)
            pg = AG[rows, :]
            HC[m, rows, mine] = (pg * sigmoid(pg) * AU[rows, :]).astype(BF)

        send(HC.at[m, :, mine], HC.at[m, :, mine], h_s.at[0], h_r.at[m, 0], {"c": oc})

    def back(m):
        HG[...] = jnp.zeros_like(HG)

        @pl.loop(0, 4)
        def _(k):
            HG[...] += dot_nt(G[2 * m + 1, :, lanes(k, 1024)], wd[:, lanes(k, 1024)])

        @pl.loop(0, 6)
        def _(i):
            rows = lanes(i, 64)
            pg, pu, hr = AG[rows, :], AU[rows, :], HG[rows, :]
            g = gcol[m, rows, 0:1]
            sig = sigmoid(pg)
            act = pg * sig
            hw = HC[m, rows, mine].astype(F32)
            dcol[m, rows, :] = jnp.broadcast_to(jnp.sum(hw * hr, axis=1, keepdims=True), (64, BLK))
            hs = hr * g
            PG[m, rows, mine] = (hs * pu * (sig * (1.0 + pg * (1.0 - sig)))).astype(BF)
            PU[m, rows, mine] = (hs * act).astype(BF)
            HS[m, rows, :] = (hw * g).astype(BF)

        for n, buf in enumerate((PG, PU)):
            send(buf.at[m, :, mine], buf.at[m, :, mine], h_s.at[0], h_r.at[m, 1 + n], {"c": oc})

    def spot(p, x_):
        return lanes(rem(zl + TURN[p], 4) * 4 + x_)

    def far_sends(a):
        for p in range(4):
            to = right if p % 2 == 0 else left
            send(Pt.at[a, :, spot(p, far)], FX.at[a, p], rx_s.at[0], rf_r.at[a, p], {"x": to})

    def near_sends(a, ps=(0, 1, 2, 3)):
        for p in ps:
            if p % 2 == 0:
                send(Pt.at[a, :, spot(p, left)], XR.at[a, p], rx_s.at[0], rr_r.at[a, p], {"x": left})
            else:
                send(Pt.at[a, :, spot(p, right)], XL.at[a, p], rx_s.at[0], rl_r.at[a, p], {"x": right})

    def outs(m):
        wait(HC.at[m, :, 0:HID], h_r.at[m, 0])

        @pl.loop(0, 4)
        def _(q):
            Pt[2 * m, :, lanes(q, 512)] = dot(HC[m], WdH[:, lanes(q, 512)]).astype(BF)

    def ins(m):
        wait(PG.at[m, :, 0:HID], h_r.at[m, 1])
        wait(PU.at[m, :, 0:HID], h_r.at[m, 2])

        @pl.loop(0, 4)
        def _(q):
            at = lanes(q, 512)
            Pt[2 * m + 1, :, at] = (dot_nt(PG[m], WgH[at, :]) + dot_nt(PU[m], WuH[at, :])).astype(BF)

    def second_sends(a, ps=(0, 1, 2, 3)):
        for p in ps:
            wait(FX.at[a, p], rf_r.at[a, p])
            tx = right if p % 2 == 0 else left
            here = spot(p, tx)
            Pt[a, :, here] = (Pt[a, :, here].astype(F32) + FX[a, p].astype(F32)).astype(BF)
            if p % 2 == 0:
                send(Pt.at[a, :, here], XL.at[a, p], rx_s.at[0], rl_r.at[a, p], {"x": right})
            else:
                send(Pt.at[a, :, here], XR.at[a, p], rx_s.at[0], rr_r.at[a, p], {"x": left})

    def third_sends(a, ps=(0, 1, 2, 3)):
        for p in ps:
            wait(XL.at[a, p], rl_r.at[a, p])
            wait(XR.at[a, p], rr_r.at[a, p])
            total = Pt[a, :, spot(p, x)].astype(F32)
            total = total + XL[a, p].astype(F32) + XR[a, p].astype(F32)
            zp = rem(zl + TURN[p], 4)
            for h in range(2):
                to = h * 4 + zp
                rows = total[h * HALF : (h + 1) * HALF, :]

                def keep():
                    zo[a, h] = rows
                    zo[a, 1 - h] = jnp.zeros((HALF, BLK), F32)

                def pass_on():
                    zs[a, 2 * p + h] = rows.astype(BF)
                    step = rem(z + 8 - to, 8)
                    send(zs.at[a, 2 * p + h], zr.at[a, step - 1], rz_s.at[0], rz_r.at[a], {"zh": h, "zl": zp})

                if TURN[p] == 0:
                    pl.when(zh == h)(keep)
                    pl.when(zh != h)(pass_on)
                else:
                    pass_on()

    def finish(a):
        wait(zr.at[a], rz_r.at[a])
        for step in range(1, 8):
            zo[a, rem(z + step, 8) // 4] += zr[a, step - 1].astype(F32)
        for h in range(2):
            fin[a, h] = zo[a, h].astype(BF)
            ret[a, cap(h * 4 + y), :] = fin[a, h, cap(y), :]
        for dy in range(1, 4):
            ty = rem(y + dy, 4)
            for h in range(2):
                send(fin.at[a, h, cap(ty), :], ret.at[a, cap(h * 4 + y), :], b_s.at[0], b_r.at[a], {"y": ty})

    def send_dots():
        @pl.loop(0, 8)
        def _(s):
            dts[s] = tile_of([to_row(dcol[m, cap(s), :]) for m in range(2)])

        dtr[e] = dts[e]
        for dz, dy in PEERS:
            tz, ty = rem(zh + dz, 2), rem(y + dy, 4)
            send(dts.at[tz * 4 + ty], dtr.at[e], dt_s.at[0], dt_r.at[0], {"zh": tz, "y": ty})

    def take_dots():
        wait(dts.at[0:7], dt_r.at[0])
        rows = []
        for m in range(2):
            total = jnp.zeros((BLK, BLK), F32)
            for ex in range(8):
                at = lane + float(ex * CAP)
                row = dtr[ex][m : m + 1, :]
                total = total + jnp.where(slots[m, 0] == at, row, 0.0) - jnp.where(slots[m, 1] == at, row, 0.0)
            rows.append(to_row(jnp.sum(total, axis=1, keepdims=True)))
        arS[1, 0] = tile_of(rows)
        ar_one(1)

    def weight_grads(lo, hi):
        @pl.loop(lo, hi)
        def _(i):
            at = lanes(i, 512)
            t0, t1 = G[0, :, at], G[2, :, at]
            wg[at, :] = (dot_tn(t0, PG[0, :, mine]) + dot_tn(t1, PG[1, :, mine])).astype(BF)
            wu[at, :] = (dot_tn(t0, PU[0, :, mine]) + dot_tn(t1, PU[1, :, mine])).astype(BF)
            wd[:, at] = (dot_tn(HS[0], G[1, :, at]) + dot_tn(HS[1], G[3, :, at])).astype(BF)

    def send_router():
        total = ar_end(1)
        share = jnp.zeros((BLK, BLK), F32)
        deltas = []
        for m in range(2):
            _, _, h0, h1 = hits(m)
            delta = to_col(total[m : m + 1, :], BLK) * gates[m, 0] * gates[m, 1]
            deltas.append(delta)
            share = share + lax.dot_general(
                delta * (h0 - h1), tok[m].astype(F32), (((0,), (0,)), ((), ())),
                preferred_element_type=F32, precision=lax.Precision.HIGHEST,
            )
        rgs[...] = share[0:8, :]
        for n, (dz, dy) in enumerate(PEERS):
            tz, ty = rem(zh + dz, 2), rem(y + dy, 4)
            send(rgs, rgr.at[n], rg_s.at[0], rg_r.at[0], {"zh": tz, "y": ty})
        return deltas

    stage_a(0)
    stage_a(1)
    b_start()
    stage_a(2)
    ar_two(0)
    stage_b(0)
    b_forward()
    ar_three(0)
    stage_c(0)
    make_gates()
    b_spread()
    stage_b(1)
    stage_d(0)
    stage_c(1)
    stage_b(2)
    stage_e(0)
    for k, buf in enumerate((wg, wu, wd)):
        pltpu.make_async_copy(buf, buf, w_l.at[k]).wait()
    for k, half in enumerate((WgH.at[:, 0:HID], WuH.at[:, 0:HID], WdH.at[0:HID, :])):
        wait(half, w_l.at[3 + k])
        wait(half, w_r.at[k])
    pre(0)
    hid(0)
    stage_d(1)
    stage_e(1)
    take_gates()
    back(0)
    stage_c(2)
    outs(0)
    far_sends(0)
    near_sends(0)
    ins(0)
    stage_d(2)
    far_sends(1)
    second_sends(0)
    near_sends(1)
    b_take(0)
    stage_e(2)
    pre(1)
    hid(1)
    b_take(1)
    outs(1)
    second_sends(1)
    far_sends(2)
    near_sends(2)
    b_take(2)
    b_take(3)
    third_sends(0)
    stage_e(3)
    back(1)
    send_dots()
    ins(1)
    third_sends(1)
    second_sends(2)
    far_sends(3)
    near_sends(3, (0,))
    take_dots()
    weight_grads(0, 3)
    finish(0)
    third_sends(2)
    second_sends(3, (0,))
    near_sends(3, (1,))
    second_sends(3, (1,))
    near_sends(3, (2,))
    ar_two(1)
    second_sends(3, (2,))
    near_sends(3, (3,))
    second_sends(3, (3,))
    weight_grads(3, 5)
    finish(1)
    third_sends(3, (0,))
    third_sends(3, (1,))
    third_sends(3, (2,))
    ar_three(1)
    third_sends(3, (3,))
    weight_grads(5, 6)
    deltas = send_router()
    weight_grads(6, 8)
    finish(2)
    finish(3)

    for m in range(2):
        a = 2 * m
        wait(ret.at[a, 0:288, :], b_r.at[a])
        wait(ret.at[a + 1, 0:288, :], b_r.at[a + 1])
        one = jnp.zeros((BLK, BLK), F32)
        two = jnp.zeros((BLK, BLK), F32)
        grad = deltas[m] * dmat[m]
        for q in range(3):
            at = lane + float(q * BLK)
            p0 = jnp.where(slots[m, 0] == at, 1.0, 0.0)
            p1 = jnp.where(slots[m, 1] == at, 1.0, 0.0)
            rows = ret[a, q * BLK : (q + 1) * BLK, :]
            one = one + dot(p0.astype(BF), rows)
            two = two + dot(p1.astype(BF), rows)
            grad = grad + dot((p0 + p1).astype(BF), ret[a + 1, q * BLK : (q + 1) * BLK, :])
        mixed[m] = (gates[m, 0] * one + gates[m, 1] * two).astype(BF)
        tgrad[m] = grad.astype(BF)

    whole = rgs[...]
    wait(rgr.at[0:7], rg_r.at[0])
    for n in range(7):
        whole = whole + rgr[n]
    rg[...] = whole

    wait(snd.at[:, 0:288, :], a_s.at[0])
    wait(G.at[0:3, 0:HALF, 0:896], z_s.at[0])
    wait(G.at[0:3, :, 0:1536], x_s.at[0])
    wait(G.at[:, :, 0:2048], d_s.at[0])
    wait(Pt.at[:, :, 0:1536], rx_s.at[0])
    wait(zr, rz_s.at[0])
    wait(ret.at[:, 0:288, :], b_s.at[0])
    wait(zr.at[0, 0:6], xb_s.at[0])
    wait(G.at[3, 0:HALF, 0:3584], z3_s.at[0])
    for k, half in enumerate((WgH.at[:, 0:HID], WuH.at[:, 0:HID], WdH.at[0:HID, :])):
        wait(half, w_s.at[k])
    wait(G.at[0, :, 0:1536], h_s.at[0])
    wait(arR, ar_s.at[0])
    wait(gts.at[0:7], gt_s.at[0])
    wait(dts.at[0:7], dt_s.at[0])
    wait(rgr.at[0:7], rg_s.at[0])


def write_out(*refs):
    sems = refs[12]
    copies = [pltpu.make_async_copy(refs[k], refs[6 + k], sems.at[k]) for k in range(6)]
    for copy in copies:
        copy.start()
    for copy in copies:
        copy.wait()


def shards(tokens, expert_ids, router_weight, w_gate, w_up, w_down, cotangent):
    big = lambda *dims: pltpu.VMEM(dims, BF)
    wide = lambda *dims: pltpu.VMEM(dims, F32)
    dma = lambda *dims: pltpu.SemaphoreType.DMA(dims)
    vm = pl.BlockSpec(memory_space=pltpu.VMEM)
    anyw = pl.BlockSpec(memory_space=pl.ANY)
    D = 4096
    results = pl.pallas_call(
        kernel,
        name="expert_layer",
        out_shape=(
            big(2, BLK, BLK), big(2, BLK, BLK), big(D, HID), big(D, HID), big(HID, D), wide(8, BLK),
        ),
        in_specs=[vm, vm, vm, vm, anyw, anyw, anyw],
        out_specs=(vm,) * 6,
        scratch_shapes=[
            big(4, ROWS, D),
            big(2048, 512), big(2048, 512), big(512, 2048), big(4, ROWS, BLK), big(4, 2, HALF, BLK), big(3, 2, HALF, BLK),
            wide(ROWS, HID), wide(ROWS, HID), wide(ROWS, HID),
            big(2, ROWS, 512), big(2, ROWS, 512), big(2, ROWS, 512), big(2, ROWS, HID),
            wide(2, ROWS, BLK), wide(2, ROWS, BLK),
            big(4, ROWS, 2048), big(4, 4, ROWS, BLK), big(4, 4, ROWS, BLK), big(4, 4, ROWS, BLK),
            big(4, 8, HALF, BLK), big(4, 7, HALF, BLK), wide(4, 2, HALF, BLK), big(4, 2, HALF, BLK), big(4, ROWS, BLK),
            wide(2, 2, BLK, BLK), wide(2, 2, BLK, BLK), wide(2, BLK, BLK),
            wide(2, 3, 8, BLK), wide(2, 7, 8, BLK), wide(8, 8, BLK), wide(8, 8, BLK), wide(8, 8, BLK), wide(8, 8, BLK),
            wide(8, BLK), wide(7, 8, BLK),
            dma(6), dma(3), dma(3), dma(1), dma(4), dma(1), dma(3, 8), dma(1), dma(3, 8), dma(3, 8), dma(3, 8),
            dma(1), dma(4), dma(1), dma(2, 3),
            dma(1), dma(4, 4), dma(4, 4), dma(4, 4), dma(1), dma(4), dma(1), dma(4),
            dma(1), dma(2, 3), dma(1), dma(1), dma(1), dma(1), dma(1), dma(1), dma(1), dma(4), dma(1), dma(4),
        ],
        compiler_params=pltpu.CompilerParams(
            collective_id=0, has_side_effects=True, vmem_limit_bytes=52 * 1024 * 1024
        ),
    )(tokens, cotangent, expert_ids.transpose(0, 2, 1), router_weight.T, w_gate[0], w_up[0], w_down[0])
    mixed, tgrad, gg, ug, dg, rg = pl.pallas_call(
        write_out,
        name="write_out",
        out_shape=tuple(jax.ShapeDtypeStruct(v.shape, v.dtype) for v in results),
        in_specs=[vm] * 6,
        out_specs=(anyw,) * 6,
        scratch_shapes=[dma(6)],
        compiler_params=pltpu.CompilerParams(vmem_limit_bytes=1024 * 1024),
    )(*(pltpu.with_memory_space_constraint(v, pltpu.VMEM) for v in results))
    return mixed, tgrad, gg[None], ug[None], dg[None], rg.T


def solution(mesh):
    split = Mesh(mesh.devices.reshape(4, 4, 2, 2, 4), REP + EP)
    in_specs = (
        P(None, EP, REP),
        P(None, EP, None),
        P(REP, None),
        P(EP, None, REP),
        P(EP, None, REP),
        P(EP, REP, None),
        P(None, EP, REP),
    )
    out_specs = (
        P(None, EP, REP),
        P(None, EP, REP),
        P(EP, None, REP),
        P(EP, None, REP),
        P(EP, REP, None),
        P(REP, None),
    )
    return jax.shard_map(shards, mesh=split, in_specs=in_specs, out_specs=out_specs, check_vma=False)
```

```python
import jax
import jax.numpy as jnp
from jax import lax
from jax.experimental import pallas as pl
from jax.experimental.pallas import tpu as pltpu
from jax.sharding import Mesh
from jax.sharding import PartitionSpec as P

MESH = pl.DeviceIdType.MESH
REP = ("zl", "x", "c")
EP = ("zh", "y")
F32 = jnp.float32
BF = jnp.bfloat16
CAP = 48
ROWS = 384
BLK = 128
HID = 256
PEERS = [(dz, dy) for dz in range(2) for dy in range(4) if dz or dy]
HALF = 192
TURN = (0, 1, 3, 2)
NEAR = (0, 1, 7, 2, 6, 3, 5, 4)


def rem(value, n):
    return lax.rem(value, jnp.int32(n))


def wait(ref, sem):
    pltpu.make_async_copy(ref, ref, sem).wait()


def dot(a, b):
    return jnp.dot(a, b, preferred_element_type=F32)


def dot_tn(a, b):
    return lax.dot_general(a, b, (((0,), (0,)), ((), ())), preferred_element_type=F32)


def dot_nt(a, b):
    return lax.dot_general(a, b, (((1,), (1,)), ((), ())), preferred_element_type=F32)


def iota(rows, lanes, dim):
    return lax.broadcasted_iota(jnp.int32, (rows, lanes), dim).astype(F32)


def to_row(col):
    n = col.shape[0]
    return jnp.sum(jnp.where(iota(n, BLK, 0) == iota(n, BLK, 1), col, 0.0), axis=0, keepdims=True)


def to_col(row, n):
    return jnp.sum(jnp.where(iota(n, BLK, 0) == iota(n, BLK, 1), row, 0.0), axis=1, keepdims=True)


def tile_of(rows):
    sub = iota(8, BLK, 0)
    return jnp.where(sub == 0.0, rows[0], 0.0) + jnp.where(sub == 1.0, rows[1], 0.0)


def sigmoid(v):
    return 1.0 / (1.0 + jnp.exp(-v))


def kernel(
    tok, cot, ids, rwt, wg_h, wu_h, wd_h,
    mixed, tgrad, wg, wu, wd, rg,
    G, WgH, WuH, WdH, snd, HB, XB, HX, AG, AU, HG, HC, PG, PU, HS, gcol, dcol,
    Pt, FX, XL, XR, zs, zr, zo, fin, ret, slots, gates, dmat, arS, arR, gts, gtr, dts, dtr, rgs, rgr,
    w_l, w_s, w_r, a_s, a_r, z_s, z_r, x_s, xl_r, xr_r, f_r, d_s, d_r, h_s, h_r,
    rx_s, rf_r, rl_r, rr_r, rz_s, rz_r, b_s, b_r, ar_s, ar_r, gt_s, gt_r, dt_s, dt_r, rg_s, rg_r, xb_s, xb_r, z3_s, z3_r, by_s, by_r,
):
    zl = lax.axis_index("zl")
    x = lax.axis_index("x")
    c = lax.axis_index("c")
    zh = lax.axis_index("zh")
    y = lax.axis_index("y")
    right, left, far = rem(x + 1, 4), rem(x + 3, 4), rem(x + 2, 4)
    z = zh * 4 + zl
    e = zh * 4 + y
    oc = 1 - c
    r = zl * 8 + x * 2 + c

    def send(src, dst, ss, rs, dev):
        pltpu.make_async_remote_copy(
            src_ref=src, dst_ref=dst, send_sem=ss, recv_sem=rs, device_id=dev, device_id_type=MESH
        ).start()

    def lanes(index, width=BLK):
        return pl.ds(pl.multiple_of(index * width, width), width)

    def feat(zl_, x_, c_):
        return zl_ * 8 + x_ * 2 + c_

    def col(arr, zl_, x_):
        return G.at[arr, :, lanes(feat(zl_, x_, c))]

    def cap(index):
        return pl.ds(pl.multiple_of(index * CAP, 16), CAP)

    mine = lanes(c, HID)

    barrier = pltpu.get_barrier_semaphore()
    pl.semaphore_signal(barrier, inc=1, device_id={"c": oc}, device_id_type=MESH)
    for j in range(1, 4):
        pl.semaphore_signal(barrier, inc=1, device_id={"x": rem(x + j, 4)}, device_id_type=MESH)
        pl.semaphore_signal(barrier, inc=1, device_id={"zl": rem(zl + j, 4)}, device_id_type=MESH)
    for j in range(1, 4):
        dev = {"zh": 1 - zh, "zl": rem(zl + j, 4)}
        pl.semaphore_signal(barrier, inc=1, device_id=dev, device_id_type=MESH)
    for dz, dy in PEERS:
        dev = {"zh": rem(zh + dz, 2), "y": rem(y + dy, 4)}
        pl.semaphore_signal(barrier, inc=1, device_id=dev, device_id_type=MESH)

    sub, lane = iota(BLK, BLK, 0), iota(BLK, BLK, 1)

    def hits(m):
        both = ids[m].astype(F32)
        first, second = to_col(both[0:1, :], BLK), to_col(both[1:2, :], BLK)
        return first, second, jnp.where(first == lane, 1.0, 0.0), jnp.where(second == lane, 1.0, 0.0)

    def route(m):
        first, second, h0, h1 = hits(m)
        tri = jnp.where(lane < sub, 1.0, 0.0).astype(BF)
        before = dot(tri, (h0 + h1).astype(BF))
        s0 = first * float(CAP) + jnp.sum(h0 * before, axis=1, keepdims=True)
        s1 = second * float(CAP) + jnp.sum(h1 * before, axis=1, keepdims=True)
        slots[m, 0] = jnp.broadcast_to(s0, (BLK, BLK))
        slots[m, 1] = jnp.broadcast_to(s1, (BLK, BLK))
        at = iota(ROWS, BLK, 0)
        match = jnp.where((at == to_row(s0)) | (at == to_row(s1)), 1.0, 0.0).astype(BF)
        for n, rows in enumerate((tok, cot)):
            arr = 2 * m + n
            snd[arr] = dot(match, rows[m]).astype(BF)
            for h in range(2):
                HB[arr, h, cap(y), :] = snd[arr, cap(h * 4 + y), :]

    def logits(m):
        _, _, h0, h1 = hits(m)
        diff = jnp.zeros((BLK, BLK), F32)
        for ex in range(8):
            diff = diff + (h0 - h1)[:, ex : ex + 1] * rwt[ex : ex + 1, :].astype(F32)
        dmat[m] = diff
        return to_row(jnp.sum(tok[m].astype(F32) * diff, axis=1, keepdims=True))

    def y_sends(*arrs):
        for arr in arrs:
            for dy in range(1, 4):
                ty = rem(y + dy, 4)
                for h in range(2):
                    send(snd.at[arr, cap(h * 4 + ty), :], HB.at[arr, h, cap(y), :],
                         a_s.at[0], a_r.at[arr], {"y": ty})

    route(0)
    pl.semaphore_wait(barrier, 17)

    def ar_one(k):
        for j in range(1, 4):
            send(arS.at[k, 0], arR.at[k, j - 1], ar_s.at[0], ar_r.at[k, 0], {"zl": rem(zl + j, 4)})

    def ar_two(k):
        total = arS[k, 0]
        wait(arR.at[k, 0:3], ar_r.at[k, 0])
        for j in range(3):
            total = total + arR[k, j]
        arS[k, 1] = total
        for j in range(1, 4):
            send(arS.at[k, 1], arR.at[k, 2 + j], ar_s.at[0], ar_r.at[k, 1], {"x": rem(x + j, 4)})

    def ar_three(k):
        total = arS[k, 1]
        wait(arR.at[k, 3:6], ar_r.at[k, 1])
        for j in range(3, 6):
            total = total + arR[k, j]
        arS[k, 2] = total
        send(arS.at[k, 2], arR.at[k, 6], ar_s.at[0], ar_r.at[k, 2], {"c": oc})

    def ar_end(k):
        wait(arR.at[k, 6], ar_r.at[k, 2])
        return arS[k, 2] + arR[k, 6]


    y_sends(0, 1)
    arS[0, 0] = tile_of([logits(0), logits(1)])
    ar_one(0)
    route(1)
    send(snd.at[3], XB.at[0], xb_s.at[0], xb_r.at[0], {"x": right})
    send(snd.at[3], XB.at[1], xb_s.at[0], xb_r.at[1], {"x": left})
    y_sends(2)

    pltpu.make_async_copy(wg_h, wg, w_l.at[0]).start()
    pltpu.make_async_copy(wu_h, wu, w_l.at[1]).start()
    pltpu.make_async_copy(wd_h, wd, w_l.at[2]).start()

    @pl.loop(0, 16)
    def _(b):
        at = feat(b // 4, b % 4, c)
        pltpu.make_async_copy(wg_h.at[lanes(at), :], WgH.at[lanes(b), mine], w_l.at[3]).start()
        pltpu.make_async_copy(wu_h.at[lanes(at), :], WuH.at[lanes(b), mine], w_l.at[4]).start()
        pltpu.make_async_copy(wd_h.at[:, lanes(at)], WdH.at[mine, lanes(b)], w_l.at[5]).start()

    @pl.loop(0, 16)
    def _(b):
        at = feat(b // 4, b % 4, oc)
        send(wg_h.at[lanes(at), :], WgH.at[lanes(b), mine], w_s.at[0], w_r.at[0], {"c": oc})
        send(wu_h.at[lanes(at), :], WuH.at[lanes(b), mine], w_s.at[1], w_r.at[1], {"c": oc})
        send(wd_h.at[:, lanes(at)], WdH.at[mine, lanes(b)], w_s.at[2], w_r.at[2], {"c": oc})

    def place(arr, z8, x_):
        return G.at[arr, pl.ds(pl.multiple_of(z8 // 4 * HALF, HALF), HALF), lanes(feat(rem(z8, 4), x_, c))]

    def spread_block(arr, z8, j):
        here = place(arr, z8, x)
        send(here, here, x_s.at[0], xl_r.at[arr, j], {"x": right})
        send(here, here, x_s.at[0], xr_r.at[arr, j], {"x": left})
        send(here, here, d_s.at[0], d_r.at[arr], {"c": oc})

    def at_z(z8):
        return {"zh": z8 // 4, "zl": rem(z8, 4)}

    def stage_a(arr):
        wait(snd.at[arr, 0:288, :], a_r.at[arr])
        here = place(arr, z, x)
        for j in range(1, 8):
            to = rem(z + 8 - NEAR[j], 8)
            send(HB.at[arr, to // 4], here, z_s.at[0], z_r.at[arr, j], at_z(to))
        here[...] = HB[arr, zh]
        spread_block(arr, z, 0)

    def stage_b(arr):
        for j in range(1, 8):
            zj = rem(z + NEAR[j], 8)
            wait(place(arr, zj, x), z_r.at[arr, j])
            spread_block(arr, zj, j)

    def stage_c(arr):
        for j in range(8):
            zj = rem(z + NEAR[j], 8)
            here = place(arr, zj, left)
            wait(here, xl_r.at[arr, j])
            if j % 2 == 0:
                send(here, here, x_s.at[0], f_r.at[arr, j], {"x": right})
            send(here, here, d_s.at[0], d_r.at[arr], {"c": oc})
            here = place(arr, zj, right)
            wait(here, xr_r.at[arr, j])
            if j % 2 == 1:
                send(here, here, x_s.at[0], f_r.at[arr, j], {"x": left})
            send(here, here, d_s.at[0], d_r.at[arr], {"c": oc})

    def b_forward():
        wait(XB.at[0], xb_r.at[0])
        send(XB.at[0, 0:HALF, :], XB.at[2, 0:HALF, :], xb_s.at[0], xb_r.at[2], {"x": right})
        wait(XB.at[1], xb_r.at[1])
        send(XB.at[1, HALF:, :], XB.at[2, HALF:, :], xb_s.at[0], xb_r.at[3], {"x": left})

    def b_y(q):
        src = snd.at[3] if q == 0 else XB.at[q - 1]
        for h in range(2):
            if q > 0:
                HX[q, h, cap(y), :] = src[cap(h * 4 + y), :]
            else:
                HX[q, h, cap(y), :] = HB[3, h, cap(y), :]
        for dy in range(1, 4):
            ty = rem(y + dy, 4)
            for h in range(2):
                send(src.at[cap(h * 4 + ty), :], HX.at[q, h, cap(y), :], by_s.at[0], by_r.at[q], {"y": ty})

    def b_far():
        wait(XB.at[2, 0:HALF, :], xb_r.at[2])
        wait(XB.at[2, HALF:, :], xb_r.at[3])
        b_y(3)

    def b_out(q, src, x_):
        here = place(3, z, x_)
        for j in range(1, 8):
            to = rem(z + 8 - NEAR[j], 8)
            send(src.at[to // 4], here, z3_s.at[0], z3_r.at[q], at_z(to))
        here[...] = src[zh]
        send(here, here, d_s.at[0], d_r.at[3], {"c": oc})

    def b_spread():
        for q, x_ in enumerate((x, left, right, far)):
            wait(snd.at[3, 0:288, :], by_r.at[q])
            b_out(q, HX.at[q], x_)

    def b_take(q):
        wait(zr.at[0], z3_r.at[q])
        for j in range(1, 8):
            here = place(3, rem(z + NEAR[j], 8), (x, left, right, far)[q])
            send(here, here, d_s.at[0], d_r.at[3], {"c": oc})

    def stage_d(arr):
        for j in range(8):
            here = place(arr, rem(z + NEAR[j], 8), far)
            wait(here, f_r.at[arr, j])
            send(here, here, d_s.at[0], d_r.at[arr], {"c": oc})

    def stage_e(arr):
        wait(G.at[arr, :, 0:2048], d_r.at[arr])

    def make_gates():
        total = ar_end(0)
        for m in range(2):
            diff = to_col(total[m : m + 1, :], BLK)
            gates[m, 0] = jnp.broadcast_to(sigmoid(diff), (BLK, BLK))
            gates[m, 1] = jnp.broadcast_to(sigmoid(-diff), (BLK, BLK))

        @pl.loop(0, 8)
        def _(ex):
            at = lane + (ex * CAP).astype(F32)
            rows = []
            for m in range(2):
                picked = jnp.where(slots[m, 0] == at, gates[m, 0], 0.0)
                picked = picked + jnp.where(slots[m, 1] == at, gates[m, 1], 0.0)
                rows.append(jnp.sum(picked, axis=0, keepdims=True))
            gts[ex] = tile_of(rows)

        gtr[e] = gts[e]
        for n, (dz, dy) in enumerate(PEERS):
            tz, ty = rem(zh + dz, 2), rem(y + dy, 4)
            send(gts.at[tz * 4 + ty], gtr.at[e], gt_s.at[0], gt_r.at[0], {"zh": tz, "y": ty})

    def take_gates():
        wait(gts.at[0:7], gt_r.at[0])

        @pl.loop(0, 8)
        def _(s):
            tile = gtr[s]
            for m in range(2):
                gcol[m, cap(s), :] = jnp.broadcast_to(to_col(tile[m : m + 1, :], CAP), (CAP, BLK))

    def pre(m):
        AG[...] = jnp.zeros_like(AG)
        AU[...] = jnp.zeros_like(AU)

        @pl.loop(0, 4)
        def _(k):
            rows = G[2 * m, :, lanes(k, 1024)]
            AG[...] += dot(rows, wg[lanes(k, 1024), :])
            AU[...] += dot(rows, wu[lanes(k, 1024), :])

    def hid(m):
        @pl.loop(0, 6)
        def _(i):
            rows = lanes(i, 64)
            pg = AG[rows, :]
            HC[m, rows, mine] = (pg * sigmoid(pg) * AU[rows, :]).astype(BF)

        send(HC.at[m, :, mine], HC.at[m, :, mine], h_s.at[0], h_r.at[m, 0], {"c": oc})

    def back(m):
        HG[...] = jnp.zeros_like(HG)

        @pl.loop(0, 4)
        def _(k):
            HG[...] += dot_nt(G[2 * m + 1, :, lanes(k, 1024)], wd[:, lanes(k, 1024)])

        @pl.loop(0, 6)
        def _(i):
            rows = lanes(i, 64)
            pg, pu, hr = AG[rows, :], AU[rows, :], HG[rows, :]
            g = gcol[m, rows, 0:1]
            sig = sigmoid(pg)
            act = pg * sig
            hw = HC[m, rows, mine].astype(F32)
            dcol[m, rows, :] = jnp.broadcast_to(jnp.sum(hw * hr, axis=1, keepdims=True), (64, BLK))
            hs = hr * g
            PG[m, rows, mine] = (hs * pu * (sig * (1.0 + pg * (1.0 - sig)))).astype(BF)
            PU[m, rows, mine] = (hs * act).astype(BF)
            HS[m, rows, :] = (hw * g).astype(BF)

        for n, buf in enumerate((PG, PU)):
            send(buf.at[m, :, mine], buf.at[m, :, mine], h_s.at[0], h_r.at[m, 1 + n], {"c": oc})

    def spot(p, x_):
        return lanes(rem(zl + TURN[p], 4) * 4 + x_)

    def far_sends(a):
        for p in range(4):
            to = right if p % 2 == 0 else left
            send(Pt.at[a, :, spot(p, far)], FX.at[a, p], rx_s.at[0], rf_r.at[a, p], {"x": to})

    def near_sends(a, ps=(0, 1, 2, 3)):
        for p in ps:
            if p % 2 == 0:
                send(Pt.at[a, :, spot(p, left)], XR.at[a, p], rx_s.at[0], rr_r.at[a, p], {"x": left})
            else:
                send(Pt.at[a, :, spot(p, right)], XL.at[a, p], rx_s.at[0], rl_r.at[a, p], {"x": right})

    def outs(m):
        wait(HC.at[m, :, 0:HID], h_r.at[m, 0])

        @pl.loop(0, 4)
        def _(q):
            Pt[2 * m, :, lanes(q, 512)] = dot(HC[m], WdH[:, lanes(q, 512)]).astype(BF)

    def ins(m):
        wait(PG.at[m, :, 0:HID], h_r.at[m, 1])
        wait(PU.at[m, :, 0:HID], h_r.at[m, 2])

        @pl.loop(0, 4)
        def _(q):
            at = lanes(q, 512)
            Pt[2 * m + 1, :, at] = (dot_nt(PG[m], WgH[at, :]) + dot_nt(PU[m], WuH[at, :])).astype(BF)

    def second_sends(a, ps=(0, 1, 2, 3)):
        for p in ps:
            wait(FX.at[a, p], rf_r.at[a, p])
            tx = right if p % 2 == 0 else left
            here = spot(p, tx)
            Pt[a, :, here] = (Pt[a, :, here].astype(F32) + FX[a, p].astype(F32)).astype(BF)
            if p % 2 == 0:
                send(Pt.at[a, :, here], XL.at[a, p], rx_s.at[0], rl_r.at[a, p], {"x": right})
            else:
                send(Pt.at[a, :, here], XR.at[a, p], rx_s.at[0], rr_r.at[a, p], {"x": left})

    def third_sends(a, ps=(0, 1, 2, 3)):
        for p in ps:
            wait(XL.at[a, p], rl_r.at[a, p])
            wait(XR.at[a, p], rr_r.at[a, p])
            total = Pt[a, :, spot(p, x)].astype(F32)
            total = total + XL[a, p].astype(F32) + XR[a, p].astype(F32)
            zp = rem(zl + TURN[p], 4)
            for h in range(2):
                to = h * 4 + zp
                rows = total[h * HALF : (h + 1) * HALF, :]

                def keep():
                    zo[a, h] = rows
                    zo[a, 1 - h] = jnp.zeros((HALF, BLK), F32)

                def pass_on():
                    zs[a, 2 * p + h] = rows.astype(BF)
                    step = rem(z + 8 - to, 8)
                    send(zs.at[a, 2 * p + h], zr.at[a, step - 1], rz_s.at[0], rz_r.at[a], {"zh": h, "zl": zp})

                if TURN[p] == 0:
                    pl.when(zh == h)(keep)
                    pl.when(zh != h)(pass_on)
                else:
                    pass_on()

    def finish(a):
        wait(zr.at[a], rz_r.at[a])
        for step in range(1, 8):
            zo[a, rem(z + step, 8) // 4] += zr[a, step - 1].astype(F32)
        for h in range(2):
            fin[a, h] = zo[a, h].astype(BF)
            ret[a, cap(h * 4 + y), :] = fin[a, h, cap(y), :]
        for dy in range(1, 4):
            ty = rem(y + dy, 4)
            for h in range(2):
                send(fin.at[a, h, cap(ty), :], ret.at[a, cap(h * 4 + y), :], b_s.at[0], b_r.at[a], {"y": ty})

    def send_dots():
        @pl.loop(0, 8)
        def _(s):
            dts[s] = tile_of([to_row(dcol[m, cap(s), :]) for m in range(2)])

        dtr[e] = dts[e]
        for dz, dy in PEERS:
            tz, ty = rem(zh + dz, 2), rem(y + dy, 4)
            send(dts.at[tz * 4 + ty], dtr.at[e], dt_s.at[0], dt_r.at[0], {"zh": tz, "y": ty})

    def take_dots():
        wait(dts.at[0:7], dt_r.at[0])
        rows = []
        for m in range(2):
            total = jnp.zeros((BLK, BLK), F32)
            for ex in range(8):
                at = lane + float(ex * CAP)
                row = dtr[ex][m : m + 1, :]
                total = total + jnp.where(slots[m, 0] == at, row, 0.0) - jnp.where(slots[m, 1] == at, row, 0.0)
            rows.append(to_row(jnp.sum(total, axis=1, keepdims=True)))
        arS[1, 0] = tile_of(rows)
        ar_one(1)

    def weight_grads(lo, hi):
        @pl.loop(lo, hi)
        def _(i):
            at = lanes(i, 512)
            t0, t1 = G[0, :, at], G[2, :, at]
            wg[at, :] = (dot_tn(t0, PG[0, :, mine]) + dot_tn(t1, PG[1, :, mine])).astype(BF)
            wu[at, :] = (dot_tn(t0, PU[0, :, mine]) + dot_tn(t1, PU[1, :, mine])).astype(BF)
            wd[:, at] = (dot_tn(HS[0], G[1, :, at]) + dot_tn(HS[1], G[3, :, at])).astype(BF)

    def send_router():
        total = ar_end(1)
        share = jnp.zeros((BLK, BLK), F32)
        deltas = []
        for m in range(2):
            _, _, h0, h1 = hits(m)
            delta = to_col(total[m : m + 1, :], BLK) * gates[m, 0] * gates[m, 1]
            deltas.append(delta)
            share = share + lax.dot_general(
                delta * (h0 - h1), tok[m].astype(F32), (((0,), (0,)), ((), ())),
                preferred_element_type=F32, precision=lax.Precision.HIGHEST,
            )
        rgs[...] = share[0:8, :]
        for n, (dz, dy) in enumerate(PEERS):
            tz, ty = rem(zh + dz, 2), rem(y + dy, 4)
            send(rgs, rgr.at[n], rg_s.at[0], rg_r.at[0], {"zh": tz, "y": ty})
        return deltas

    stage_a(0)
    stage_a(1)
    stage_a(2)
    ar_two(0)
    b_y(0)
    b_forward()
    b_y(1)
    b_y(2)
    stage_b(0)
    b_far()
    ar_three(0)
    stage_c(0)
    make_gates()
    b_spread()
    stage_b(1)
    stage_d(0)
    stage_c(1)
    stage_b(2)
    stage_e(0)
    for k, buf in enumerate((wg, wu, wd)):
        pltpu.make_async_copy(buf, buf, w_l.at[k]).wait()
    for k, half in enumerate((WgH.at[:, 0:HID], WuH.at[:, 0:HID], WdH.at[0:HID, :])):
        wait(half, w_l.at[3 + k])
        wait(half, w_r.at[k])
    pre(0)
    hid(0)
    stage_d(1)
    stage_e(1)
    take_gates()
    back(0)
    stage_c(2)
    outs(0)
    far_sends(0)
    near_sends(0)
    ins(0)
    stage_d(2)
    far_sends(1)
    second_sends(0)
    near_sends(1)
    b_take(0)
    stage_e(2)
    pre(1)
    hid(1)
    b_take(1)
    outs(1)
    second_sends(1)
    far_sends(2)
    near_sends(2)
    b_take(2)
    b_take(3)
    third_sends(0)
    stage_e(3)
    back(1)
    send_dots()
    ins(1)
    third_sends(1)
    second_sends(2)
    far_sends(3)
    near_sends(3, (0,))
    take_dots()
    weight_grads(0, 3)
    finish(0)
    third_sends(2)
    second_sends(3, (0,))
    near_sends(3, (1,))
    second_sends(3, (1,))
    near_sends(3, (2,))
    ar_two(1)
    second_sends(3, (2,))
    near_sends(3, (3,))
    second_sends(3, (3,))
    weight_grads(3, 5)
    finish(1)
    third_sends(3, (0,))
    third_sends(3, (1,))
    third_sends(3, (2,))
    ar_three(1)
    third_sends(3, (3,))
    weight_grads(5, 6)
    deltas = send_router()
    weight_grads(6, 8)
    finish(2)
    finish(3)

    for m in range(2):
        a = 2 * m
        wait(ret.at[a, 0:288, :], b_r.at[a])
        wait(ret.at[a + 1, 0:288, :], b_r.at[a + 1])
        one = jnp.zeros((BLK, BLK), F32)
        two = jnp.zeros((BLK, BLK), F32)
        grad = deltas[m] * dmat[m]
        for q in range(3):
            at = lane + float(q * BLK)
            p0 = jnp.where(slots[m, 0] == at, 1.0, 0.0)
            p1 = jnp.where(slots[m, 1] == at, 1.0, 0.0)
            rows = ret[a, q * BLK : (q + 1) * BLK, :]
            one = one + dot(p0.astype(BF), rows)
            two = two + dot(p1.astype(BF), rows)
            grad = grad + dot((p0 + p1).astype(BF), ret[a + 1, q * BLK : (q + 1) * BLK, :])
        mixed[m] = (gates[m, 0] * one + gates[m, 1] * two).astype(BF)
        tgrad[m] = grad.astype(BF)

    whole = rgs[...]
    wait(rgr.at[0:7], rg_r.at[0])
    for n in range(7):
        whole = whole + rgr[n]
    rg[...] = whole

    wait(snd.at[0:3, 0:288, :], a_s.at[0])
    wait(snd.at[:, 0:288, :], by_s.at[0])
    wait(G.at[0:3, 0:HALF, 0:896], z_s.at[0])
    wait(G.at[0:3, :, 0:1536], x_s.at[0])
    wait(G.at[:, :, 0:2048], d_s.at[0])
    wait(Pt.at[:, :, 0:1536], rx_s.at[0])
    wait(zr, rz_s.at[0])
    wait(ret.at[:, 0:288, :], b_s.at[0])
    wait(zr.at[0, 0:6], xb_s.at[0])
    wait(G.at[3, 0:HALF, 0:3584], z3_s.at[0])
    for k, half in enumerate((WgH.at[:, 0:HID], WuH.at[:, 0:HID], WdH.at[0:HID, :])):
        wait(half, w_s.at[k])
    wait(G.at[0, :, 0:1536], h_s.at[0])
    wait(arR, ar_s.at[0])
    wait(gts.at[0:7], gt_s.at[0])
    wait(dts.at[0:7], dt_s.at[0])
    wait(rgr.at[0:7], rg_s.at[0])


def write_out(*refs):
    sems = refs[12]
    copies = [pltpu.make_async_copy(refs[k], refs[6 + k], sems.at[k]) for k in range(6)]
    for copy in copies:
        copy.start()
    for copy in copies:
        copy.wait()


def shards(tokens, expert_ids, router_weight, w_gate, w_up, w_down, cotangent):
    big = lambda *dims: pltpu.VMEM(dims, BF)
    wide = lambda *dims: pltpu.VMEM(dims, F32)
    dma = lambda *dims: pltpu.SemaphoreType.DMA(dims)
    vm = pl.BlockSpec(memory_space=pltpu.VMEM)
    anyw = pl.BlockSpec(memory_space=pl.ANY)
    D = 4096
    results = pl.pallas_call(
        kernel,
        name="expert_layer",
        out_shape=(
            big(2, BLK, BLK), big(2, BLK, BLK), big(D, HID), big(D, HID), big(HID, D), wide(8, BLK),
        ),
        in_specs=[vm, vm, vm, vm, anyw, anyw, anyw],
        out_specs=(vm,) * 6,
        scratch_shapes=[
            big(4, ROWS, D),
            big(2048, 512), big(2048, 512), big(512, 2048), big(4, ROWS, BLK), big(4, 2, HALF, BLK), big(3, ROWS, BLK), big(4, 2, HALF, BLK),
            wide(ROWS, HID), wide(ROWS, HID), wide(ROWS, HID),
            big(2, ROWS, 512), big(2, ROWS, 512), big(2, ROWS, 512), big(2, ROWS, HID),
            wide(2, ROWS, BLK), wide(2, ROWS, BLK),
            big(4, ROWS, 2048), big(4, 4, ROWS, BLK), big(4, 4, ROWS, BLK), big(4, 4, ROWS, BLK),
            big(4, 8, HALF, BLK), big(4, 7, HALF, BLK), wide(4, 2, HALF, BLK), big(4, 2, HALF, BLK), big(4, ROWS, BLK),
            wide(2, 2, BLK, BLK), wide(2, 2, BLK, BLK), wide(2, BLK, BLK),
            wide(2, 3, 8, BLK), wide(2, 7, 8, BLK), wide(8, 8, BLK), wide(8, 8, BLK), wide(8, 8, BLK), wide(8, 8, BLK),
            wide(8, BLK), wide(7, 8, BLK),
            dma(6), dma(3), dma(3), dma(1), dma(3), dma(1), dma(3, 8), dma(1), dma(3, 8), dma(3, 8), dma(3, 8),
            dma(1), dma(4), dma(1), dma(2, 3),
            dma(1), dma(4, 4), dma(4, 4), dma(4, 4), dma(1), dma(4), dma(1), dma(4),
            dma(1), dma(2, 3), dma(1), dma(1), dma(1), dma(1), dma(1), dma(1), dma(1), dma(4), dma(1), dma(4), dma(1), dma(4),
        ],
        compiler_params=pltpu.CompilerParams(
            collective_id=0, has_side_effects=True, vmem_limit_bytes=52 * 1024 * 1024
        ),
    )(tokens, cotangent, expert_ids.transpose(0, 2, 1), router_weight.T, w_gate[0], w_up[0], w_down[0])
    mixed, tgrad, gg, ug, dg, rg = pl.pallas_call(
        write_out,
        name="write_out",
        out_shape=tuple(jax.ShapeDtypeStruct(v.shape, v.dtype) for v in results),
        in_specs=[vm] * 6,
        out_specs=(anyw,) * 6,
        scratch_shapes=[dma(6)],
        compiler_params=pltpu.CompilerParams(vmem_limit_bytes=1024 * 1024),
    )(*(pltpu.with_memory_space_constraint(v, pltpu.VMEM) for v in results))
    return mixed, tgrad, gg[None], ug[None], dg[None], rg.T


def solution(mesh):
    split = Mesh(mesh.devices.reshape(4, 4, 2, 2, 4), REP + EP)
    in_specs = (
        P(None, EP, REP),
        P(None, EP, None),
        P(REP, None),
        P(EP, None, REP),
        P(EP, None, REP),
        P(EP, REP, None),
        P(None, EP, REP),
    )
    out_specs = (
        P(None, EP, REP),
        P(None, EP, REP),
        P(EP, None, REP),
        P(EP, None, REP),
        P(EP, REP, None),
        P(REP, None),
    )
    return jax.shard_map(shards, mesh=split, in_specs=in_specs, out_specs=out_specs, check_vma=False)
```

```python
import jax
import jax.numpy as jnp
from jax import lax
from jax.experimental import pallas as pl
from jax.experimental.pallas import tpu as pltpu
from jax.sharding import Mesh
from jax.sharding import PartitionSpec as P

MESH = pl.DeviceIdType.MESH
REP = ("zl", "x", "c")
EP = ("zh", "y")
F32 = jnp.float32
BF = jnp.bfloat16
CAP = 48
ROWS = 384
BLK = 128
HID = 256
PEERS = [(dz, dy) for dz in range(2) for dy in range(4) if dz or dy]
HALF = 192
TURN = (0, 1, 3, 2)
NEAR = (0, 1, 7, 2, 6, 3, 5, 4)


def rem(value, n):
    return lax.rem(value, jnp.int32(n))


def wait(ref, sem):
    pltpu.make_async_copy(ref, ref, sem).wait()


def dot(a, b):
    return jnp.dot(a, b, preferred_element_type=F32)


def dot_tn(a, b):
    return lax.dot_general(a, b, (((0,), (0,)), ((), ())), preferred_element_type=F32)


def dot_nt(a, b):
    return lax.dot_general(a, b, (((1,), (1,)), ((), ())), preferred_element_type=F32)


def iota(rows, lanes, dim):
    return lax.broadcasted_iota(jnp.int32, (rows, lanes), dim).astype(F32)


def to_row(col):
    n = col.shape[0]
    return jnp.sum(jnp.where(iota(n, BLK, 0) == iota(n, BLK, 1), col, 0.0), axis=0, keepdims=True)


def to_col(row, n):
    return jnp.sum(jnp.where(iota(n, BLK, 0) == iota(n, BLK, 1), row, 0.0), axis=1, keepdims=True)


def tile_of(rows):
    sub = iota(8, BLK, 0)
    return jnp.where(sub == 0.0, rows[0], 0.0) + jnp.where(sub == 1.0, rows[1], 0.0)


def sigmoid(v):
    return 1.0 / (1.0 + jnp.exp(-v))


def kernel(
    tok, cot, ids, rwt, wg_h, wu_h, wd_h,
    mixed, tgrad, wg, wu, wd, rg,
    G, WgH, WuH, WdH, snd, HB, XB, HX, AG, AU, HG, HC, PG, PU, HS, gcol, dcol,
    Pt, FX, XL, XR, zs, zr, zo, fin, ret, slots, gates, dmat, arS, arR, gts, gtr, dts, dtr, rgs, rgr,
    w_l, w_s, w_r, a_s, a_r, z_s, z_r, x_s, xl_r, xr_r, f_r, d_s, d_r, h_s, h_r,
    rx_s, rf_r, rl_r, rr_r, rz_s, rz_r, b_s, b_r, ar_s, ar_r, gt_s, gt_r, dt_s, dt_r, rg_s, rg_r, xb_s, xb_r, z3_s, z3_r, by_s, by_r,
):
    zl = lax.axis_index("zl")
    x = lax.axis_index("x")
    c = lax.axis_index("c")
    zh = lax.axis_index("zh")
    y = lax.axis_index("y")
    right, left, far = rem(x + 1, 4), rem(x + 3, 4), rem(x + 2, 4)
    z = zh * 4 + zl
    e = zh * 4 + y
    oc = 1 - c
    r = zl * 8 + x * 2 + c

    def send(src, dst, ss, rs, dev):
        pltpu.make_async_remote_copy(
            src_ref=src, dst_ref=dst, send_sem=ss, recv_sem=rs, device_id=dev, device_id_type=MESH
        ).start()

    def lanes(index, width=BLK):
        return pl.ds(pl.multiple_of(index * width, width), width)

    def feat(zl_, x_, c_):
        return zl_ * 8 + x_ * 2 + c_

    def col(arr, zl_, x_):
        return G.at[arr, :, lanes(feat(zl_, x_, c))]

    def cap(index):
        return pl.ds(pl.multiple_of(index * CAP, 16), CAP)

    mine = lanes(c, HID)

    barrier = pltpu.get_barrier_semaphore()
    pl.semaphore_signal(barrier, inc=1, device_id={"c": oc}, device_id_type=MESH)
    for j in range(1, 4):
        pl.semaphore_signal(barrier, inc=1, device_id={"x": rem(x + j, 4)}, device_id_type=MESH)
        pl.semaphore_signal(barrier, inc=1, device_id={"zl": rem(zl + j, 4)}, device_id_type=MESH)
    for j in range(1, 4):
        dev = {"zh": 1 - zh, "zl": rem(zl + j, 4)}
        pl.semaphore_signal(barrier, inc=1, device_id=dev, device_id_type=MESH)
    for dz, dy in PEERS:
        dev = {"zh": rem(zh + dz, 2), "y": rem(y + dy, 4)}
        pl.semaphore_signal(barrier, inc=1, device_id=dev, device_id_type=MESH)

    sub, lane = iota(BLK, BLK, 0), iota(BLK, BLK, 1)

    def hits(m):
        both = ids[m].astype(F32)
        first, second = to_col(both[0:1, :], BLK), to_col(both[1:2, :], BLK)
        return first, second, jnp.where(first == lane, 1.0, 0.0), jnp.where(second == lane, 1.0, 0.0)

    def route(m):
        first, second, h0, h1 = hits(m)
        tri = jnp.where(lane < sub, 1.0, 0.0).astype(BF)
        before = dot(tri, (h0 + h1).astype(BF))
        s0 = first * float(CAP) + jnp.sum(h0 * before, axis=1, keepdims=True)
        s1 = second * float(CAP) + jnp.sum(h1 * before, axis=1, keepdims=True)
        slots[m, 0] = jnp.broadcast_to(s0, (BLK, BLK))
        slots[m, 1] = jnp.broadcast_to(s1, (BLK, BLK))
        at = iota(ROWS, BLK, 0)
        match = jnp.where((at == to_row(s0)) | (at == to_row(s1)), 1.0, 0.0).astype(BF)
        for n, rows in enumerate((tok, cot)):
            arr = 2 * m + n
            snd[arr] = dot(match, rows[m]).astype(BF)
            for h in range(2):
                HB[arr, h, cap(y), :] = snd[arr, cap(h * 4 + y), :]

    def logits(m):
        _, _, h0, h1 = hits(m)
        diff = jnp.zeros((BLK, BLK), F32)
        for ex in range(8):
            diff = diff + (h0 - h1)[:, ex : ex + 1] * rwt[ex : ex + 1, :].astype(F32)
        dmat[m] = diff
        return to_row(jnp.sum(tok[m].astype(F32) * diff, axis=1, keepdims=True))

    def y_sends(*arrs):
        for arr in arrs:
            for dy in range(1, 4):
                ty = rem(y + dy, 4)
                for h in range(2):
                    send(snd.at[arr, cap(h * 4 + ty), :], HB.at[arr, h, cap(y), :],
                         a_s.at[0], a_r.at[arr], {"y": ty})

    route(0)
    pl.semaphore_wait(barrier, 17)

    def ar_one(k):
        for j in range(1, 4):
            send(arS.at[k, 0], arR.at[k, j - 1], ar_s.at[0], ar_r.at[k, 0], {"zl": rem(zl + j, 4)})

    def ar_two(k):
        total = arS[k, 0]
        wait(arR.at[k, 0:3], ar_r.at[k, 0])
        for j in range(3):
            total = total + arR[k, j]
        arS[k, 1] = total
        for j in range(1, 4):
            send(arS.at[k, 1], arR.at[k, 2 + j], ar_s.at[0], ar_r.at[k, 1], {"x": rem(x + j, 4)})

    def ar_three(k):
        total = arS[k, 1]
        wait(arR.at[k, 3:6], ar_r.at[k, 1])
        for j in range(3, 6):
            total = total + arR[k, j]
        arS[k, 2] = total
        send(arS.at[k, 2], arR.at[k, 6], ar_s.at[0], ar_r.at[k, 2], {"c": oc})

    def ar_end(k):
        wait(arR.at[k, 6], ar_r.at[k, 2])
        return arS[k, 2] + arR[k, 6]


    y_sends(0, 1)
    arS[0, 0] = tile_of([logits(0), logits(1)])
    ar_one(0)
    route(1)
    send(snd.at[3], XB.at[0], xb_s.at[0], xb_r.at[0], {"x": right})
    send(snd.at[3], XB.at[1], xb_s.at[0], xb_r.at[1], {"x": left})
    y_sends(2)

    pltpu.make_async_copy(wg_h, wg, w_l.at[0]).start()
    pltpu.make_async_copy(wu_h, wu, w_l.at[1]).start()
    pltpu.make_async_copy(wd_h, wd, w_l.at[2]).start()

    @pl.loop(0, 16)
    def _(b):
        at = feat(b // 4, b % 4, c)
        pltpu.make_async_copy(wg_h.at[lanes(at), :], WgH.at[lanes(b), mine], w_l.at[3]).start()
        pltpu.make_async_copy(wu_h.at[lanes(at), :], WuH.at[lanes(b), mine], w_l.at[4]).start()
        pltpu.make_async_copy(wd_h.at[:, lanes(at)], WdH.at[mine, lanes(b)], w_l.at[5]).start()

    @pl.loop(0, 16)
    def _(b):
        at = feat(b // 4, b % 4, oc)
        send(wg_h.at[lanes(at), :], WgH.at[lanes(b), mine], w_s.at[0], w_r.at[0], {"c": oc})
        send(wu_h.at[lanes(at), :], WuH.at[lanes(b), mine], w_s.at[1], w_r.at[1], {"c": oc})
        send(wd_h.at[:, lanes(at)], WdH.at[mine, lanes(b)], w_s.at[2], w_r.at[2], {"c": oc})

    def place(arr, z8, x_):
        return G.at[arr, pl.ds(pl.multiple_of(z8 // 4 * HALF, HALF), HALF), lanes(feat(rem(z8, 4), x_, c))]

    def spread_block(arr, z8, j):
        here = place(arr, z8, x)
        send(here, here, x_s.at[0], xl_r.at[arr, j], {"x": right})
        send(here, here, x_s.at[0], xr_r.at[arr, j], {"x": left})
        send(here, here, d_s.at[0], d_r.at[arr], {"c": oc})

    def at_z(z8):
        return {"zh": z8 // 4, "zl": rem(z8, 4)}

    def stage_a(arr):
        wait(snd.at[arr, 0:288, :], a_r.at[arr])
        here = place(arr, z, x)
        for j in range(1, 8):
            to = rem(z + 8 - NEAR[j], 8)
            send(HB.at[arr, to // 4], here, z_s.at[0], z_r.at[arr, j], at_z(to))
        here[...] = HB[arr, zh]
        spread_block(arr, z, 0)

    def stage_b(arr):
        for j in range(1, 8):
            zj = rem(z + NEAR[j], 8)
            wait(place(arr, zj, x), z_r.at[arr, j])
            spread_block(arr, zj, j)

    def stage_c(arr):
        for j in range(8):
            zj = rem(z + NEAR[j], 8)
            here = place(arr, zj, left)
            wait(here, xl_r.at[arr, j])
            if j % 2 == 0:
                send(here, here, x_s.at[0], f_r.at[arr], {"x": right})
            send(here, here, d_s.at[0], d_r.at[arr], {"c": oc})
            here = place(arr, zj, right)
            wait(here, xr_r.at[arr, j])
            if j % 2 == 1:
                send(here, here, x_s.at[0], f_r.at[arr], {"x": left})
            send(here, here, d_s.at[0], d_r.at[arr], {"c": oc})

    def b_forward():
        wait(XB.at[0], xb_r.at[0])
        send(XB.at[0, 0:HALF, :], XB.at[2, 0:HALF, :], xb_s.at[0], xb_r.at[2], {"x": right})
        wait(XB.at[1], xb_r.at[1])
        send(XB.at[1, HALF:, :], XB.at[2, HALF:, :], xb_s.at[0], xb_r.at[3], {"x": left})

    def b_y(q):
        src = snd.at[3] if q == 0 else XB.at[q - 1]
        for h in range(2):
            if q > 0:
                HX[q, h, cap(y), :] = src[cap(h * 4 + y), :]
            else:
                HX[q, h, cap(y), :] = HB[3, h, cap(y), :]
        for dy in range(1, 4):
            ty = rem(y + dy, 4)
            for h in range(2):
                send(src.at[cap(h * 4 + ty), :], HX.at[q, h, cap(y), :], by_s.at[0], by_r.at[q], {"y": ty})

    def b_far():
        wait(XB.at[2, 0:HALF, :], xb_r.at[2])
        wait(XB.at[2, HALF:, :], xb_r.at[3])
        b_y(3)

    def b_out(q, src, x_):
        here = place(3, z, x_)
        for j in range(1, 8):
            to = rem(z + 8 - NEAR[j], 8)
            send(src.at[to // 4], here, z3_s.at[0], z3_r.at[q], at_z(to))
        here[...] = src[zh]
        send(here, here, d_s.at[0], d_r.at[3], {"c": oc})

    def b_spread():
        for q, x_ in enumerate((x, left, right, far)):
            wait(snd.at[3, 0:288, :], by_r.at[q])
            b_out(q, HX.at[q], x_)

    def b_take(q):
        wait(zr.at[0], z3_r.at[q])
        for j in range(1, 8):
            here = place(3, rem(z + NEAR[j], 8), (x, left, right, far)[q])
            send(here, here, d_s.at[0], d_r.at[3], {"c": oc})

    def stage_d(arr):
        wait(fin, f_r.at[arr])
        for j in range(8):
            here = place(arr, rem(z + NEAR[j], 8), far)
            send(here, here, d_s.at[0], d_r.at[arr], {"c": oc})

    def stage_e(arr):
        wait(G.at[arr, :, 0:2048], d_r.at[arr])

    def make_gates():
        total = ar_end(0)
        for m in range(2):
            diff = to_col(total[m : m + 1, :], BLK)
            gates[m, 0] = jnp.broadcast_to(sigmoid(diff), (BLK, BLK))
            gates[m, 1] = jnp.broadcast_to(sigmoid(-diff), (BLK, BLK))

        @pl.loop(0, 8)
        def _(ex):
            at = lane + (ex * CAP).astype(F32)
            rows = []
            for m in range(2):
                picked = jnp.where(slots[m, 0] == at, gates[m, 0], 0.0)
                picked = picked + jnp.where(slots[m, 1] == at, gates[m, 1], 0.0)
                rows.append(jnp.sum(picked, axis=0, keepdims=True))
            gts[ex] = tile_of(rows)

        gtr[e] = gts[e]
        for n, (dz, dy) in enumerate(PEERS):
            tz, ty = rem(zh + dz, 2), rem(y + dy, 4)
            send(gts.at[tz * 4 + ty], gtr.at[e], gt_s.at[0], gt_r.at[0], {"zh": tz, "y": ty})

    def take_gates():
        wait(gts.at[0:7], gt_r.at[0])

        @pl.loop(0, 8)
        def _(s):
            tile = gtr[s]
            for m in range(2):
                gcol[m, cap(s), :] = jnp.broadcast_to(to_col(tile[m : m + 1, :], CAP), (CAP, BLK))

    def pre(m):
        AG[...] = jnp.zeros_like(AG)
        AU[...] = jnp.zeros_like(AU)

        @pl.loop(0, 4)
        def _(k):
            rows = G[2 * m, :, lanes(k, 1024)]
            AG[...] += dot(rows, wg[lanes(k, 1024), :])
            AU[...] += dot(rows, wu[lanes(k, 1024), :])

    def hid(m):
        @pl.loop(0, 6)
        def _(i):
            rows = lanes(i, 64)
            pg = AG[rows, :]
            HC[m, rows, mine] = (pg * sigmoid(pg) * AU[rows, :]).astype(BF)

        send(HC.at[m, :, mine], HC.at[m, :, mine], h_s.at[0], h_r.at[m, 0], {"c": oc})

    def back(m):
        HG[...] = jnp.zeros_like(HG)

        @pl.loop(0, 4)
        def _(k):
            HG[...] += dot_nt(G[2 * m + 1, :, lanes(k, 1024)], wd[:, lanes(k, 1024)])

        @pl.loop(0, 6)
        def _(i):
            rows = lanes(i, 64)
            pg, pu, hr = AG[rows, :], AU[rows, :], HG[rows, :]
            g = gcol[m, rows, 0:1]
            sig = sigmoid(pg)
            act = pg * sig
            hw = HC[m, rows, mine].astype(F32)
            dcol[m, rows, :] = jnp.broadcast_to(jnp.sum(hw * hr, axis=1, keepdims=True), (64, BLK))
            hs = hr * g
            PG[m, rows, mine] = (hs * pu * (sig * (1.0 + pg * (1.0 - sig)))).astype(BF)
            PU[m, rows, mine] = (hs * act).astype(BF)
            HS[m, rows, :] = (hw * g).astype(BF)

        for n, buf in enumerate((PG, PU)):
            send(buf.at[m, :, mine], buf.at[m, :, mine], h_s.at[0], h_r.at[m, 1 + n], {"c": oc})

    def spot(p, x_):
        return lanes(rem(zl + TURN[p], 4) * 4 + x_)

    def far_sends(a):
        for p in range(4):
            to = right if p % 2 == 0 else left
            send(Pt.at[a, :, spot(p, far)], FX.at[a, p], rx_s.at[0], rf_r.at[a, p], {"x": to})

    def near_sends(a, ps=(0, 1, 2, 3)):
        for p in ps:
            if p % 2 == 0:
                send(Pt.at[a, :, spot(p, left)], XR.at[a, p], rx_s.at[0], rr_r.at[a, p], {"x": left})
            else:
                send(Pt.at[a, :, spot(p, right)], XL.at[a, p], rx_s.at[0], rl_r.at[a, p], {"x": right})

    def outs(m):
        wait(HC.at[m, :, 0:HID], h_r.at[m, 0])

        @pl.loop(0, 4)
        def _(q):
            Pt[2 * m, :, lanes(q, 512)] = dot(HC[m], WdH[:, lanes(q, 512)]).astype(BF)

    def ins(m):
        wait(PG.at[m, :, 0:HID], h_r.at[m, 1])
        wait(PU.at[m, :, 0:HID], h_r.at[m, 2])

        @pl.loop(0, 4)
        def _(q):
            at = lanes(q, 512)
            Pt[2 * m + 1, :, at] = (dot_nt(PG[m], WgH[at, :]) + dot_nt(PU[m], WuH[at, :])).astype(BF)

    def second_sends(a, ps=(0, 1, 2, 3)):
        for p in ps:
            wait(FX.at[a, p], rf_r.at[a, p])
            tx = right if p % 2 == 0 else left
            here = spot(p, tx)
            Pt[a, :, here] = (Pt[a, :, here].astype(F32) + FX[a, p].astype(F32)).astype(BF)
            if p % 2 == 0:
                send(Pt.at[a, :, here], XL.at[a, p], rx_s.at[0], rl_r.at[a, p], {"x": right})
            else:
                send(Pt.at[a, :, here], XR.at[a, p], rx_s.at[0], rr_r.at[a, p], {"x": left})

    def third_sends(a, ps=(0, 1, 2, 3)):
        for p in ps:
            wait(XL.at[a, p], rl_r.at[a, p])
            wait(XR.at[a, p], rr_r.at[a, p])
            total = Pt[a, :, spot(p, x)].astype(F32)
            total = total + XL[a, p].astype(F32) + XR[a, p].astype(F32)
            zp = rem(zl + TURN[p], 4)
            for h in range(2):
                to = h * 4 + zp
                rows = total[h * HALF : (h + 1) * HALF, :]

                def keep():
                    zo[a, h] = rows
                    zo[a, 1 - h] = jnp.zeros((HALF, BLK), F32)

                def pass_on():
                    zs[a, 2 * p + h] = rows.astype(BF)
                    step = rem(z + 8 - to, 8)
                    send(zs.at[a, 2 * p + h], zr.at[a, step - 1], rz_s.at[0], rz_r.at[a], {"zh": h, "zl": zp})

                if TURN[p] == 0:
                    pl.when(zh == h)(keep)
                    pl.when(zh != h)(pass_on)
                else:
                    pass_on()

    def finish(a):
        wait(zr.at[a], rz_r.at[a])
        for step in range(1, 8):
            zo[a, rem(z + step, 8) // 4] += zr[a, step - 1].astype(F32)
        for h in range(2):
            fin[a, h] = zo[a, h].astype(BF)
            ret[a, cap(h * 4 + y), :] = fin[a, h, cap(y), :]
        for dy in range(1, 4):
            ty = rem(y + dy, 4)
            for h in range(2):
                send(fin.at[a, h, cap(ty), :], ret.at[a, cap(h * 4 + y), :], b_s.at[0], b_r.at[a], {"y": ty})

    def send_dots():
        @pl.loop(0, 8)
        def _(s):
            dts[s] = tile_of([to_row(dcol[m, cap(s), :]) for m in range(2)])

        dtr[e] = dts[e]
        for dz, dy in PEERS:
            tz, ty = rem(zh + dz, 2), rem(y + dy, 4)
            send(dts.at[tz * 4 + ty], dtr.at[e], dt_s.at[0], dt_r.at[0], {"zh": tz, "y": ty})

    def take_dots():
        wait(dts.at[0:7], dt_r.at[0])
        rows = []
        for m in range(2):
            total = jnp.zeros((BLK, BLK), F32)
            for ex in range(8):
                at = lane + float(ex * CAP)
                row = dtr[ex][m : m + 1, :]
                total = total + jnp.where(slots[m, 0] == at, row, 0.0) - jnp.where(slots[m, 1] == at, row, 0.0)
            rows.append(to_row(jnp.sum(total, axis=1, keepdims=True)))
        arS[1, 0] = tile_of(rows)
        ar_one(1)

    def weight_grads(lo, hi):
        @pl.loop(lo, hi)
        def _(i):
            at = lanes(i, 512)
            t0, t1 = G[0, :, at], G[2, :, at]
            wg[at, :] = (dot_tn(t0, PG[0, :, mine]) + dot_tn(t1, PG[1, :, mine])).astype(BF)
            wu[at, :] = (dot_tn(t0, PU[0, :, mine]) + dot_tn(t1, PU[1, :, mine])).astype(BF)
            wd[:, at] = (dot_tn(HS[0], G[1, :, at]) + dot_tn(HS[1], G[3, :, at])).astype(BF)

    def send_router():
        total = ar_end(1)
        share = jnp.zeros((BLK, BLK), F32)
        deltas = []
        for m in range(2):
            _, _, h0, h1 = hits(m)
            delta = to_col(total[m : m + 1, :], BLK) * gates[m, 0] * gates[m, 1]
            deltas.append(delta)
            share = share + lax.dot_general(
                delta * (h0 - h1), tok[m].astype(F32), (((0,), (0,)), ((), ())),
                preferred_element_type=F32, precision=lax.Precision.HIGHEST,
            )
        rgs[...] = share[0:8, :]
        for n, (dz, dy) in enumerate(PEERS):
            tz, ty = rem(zh + dz, 2), rem(y + dy, 4)
            send(rgs, rgr.at[n], rg_s.at[0], rg_r.at[0], {"zh": tz, "y": ty})
        return deltas

    stage_a(0)
    stage_a(1)
    stage_a(2)
    ar_two(0)
    b_y(0)
    b_forward()
    b_y(1)
    b_y(2)
    stage_b(0)
    b_far()
    ar_three(0)
    stage_c(0)
    make_gates()
    b_spread()
    stage_b(1)
    stage_d(0)
    stage_c(1)
    stage_b(2)
    stage_e(0)
    for k, buf in enumerate((wg, wu, wd)):
        pltpu.make_async_copy(buf, buf, w_l.at[k]).wait()
    for k, half in enumerate((WgH.at[:, 0:HID], WuH.at[:, 0:HID], WdH.at[0:HID, :])):
        wait(half, w_l.at[3 + k])
        wait(half, w_r.at[k])
    pre(0)
    hid(0)
    stage_d(1)
    stage_e(1)
    take_gates()
    back(0)
    stage_c(2)
    outs(0)
    far_sends(0)
    near_sends(0)
    ins(0)
    stage_d(2)
    far_sends(1)
    second_sends(0)
    near_sends(1)
    b_take(0)
    stage_e(2)
    pre(1)
    hid(1)
    b_take(1)
    outs(1)
    second_sends(1)
    far_sends(2)
    near_sends(2)
    b_take(2)
    b_take(3)
    third_sends(0)
    stage_e(3)
    back(1)
    send_dots()
    ins(1)
    third_sends(1)
    second_sends(2)
    far_sends(3)
    near_sends(3, (0,))
    take_dots()
    weight_grads(0, 3)
    finish(0)
    third_sends(2)
    second_sends(3, (0,))
    near_sends(3, (1,))
    second_sends(3, (1,))
    near_sends(3, (2,))
    ar_two(1)
    second_sends(3, (2,))
    near_sends(3, (3,))
    second_sends(3, (3,))
    weight_grads(3, 5)
    finish(1)
    third_sends(3, (0,))
    third_sends(3, (1,))
    third_sends(3, (2,))
    ar_three(1)
    third_sends(3, (3,))
    weight_grads(5, 6)
    deltas = send_router()
    weight_grads(6, 8)
    finish(2)
    finish(3)

    for m in range(2):
        a = 2 * m
        wait(ret.at[a, 0:288, :], b_r.at[a])
        one = jnp.zeros((BLK, BLK), F32)
        two = jnp.zeros((BLK, BLK), F32)
        grad = deltas[m] * dmat[m]
        for q in range(3):
            at = lane + float(q * BLK)
            p0 = jnp.where(slots[m, 0] == at, 1.0, 0.0)
            p1 = jnp.where(slots[m, 1] == at, 1.0, 0.0)
            rows = ret[a, q * BLK : (q + 1) * BLK, :]
            one = one + dot(p0.astype(BF), rows)
            two = two + dot(p1.astype(BF), rows)
        mixed[m] = (gates[m, 0] * one + gates[m, 1] * two).astype(BF)
        wait(ret.at[a + 1, 0:288, :], b_r.at[a + 1])
        for q in range(3):
            at = lane + float(q * BLK)
            both = jnp.where((slots[m, 0] == at) | (slots[m, 1] == at), 1.0, 0.0)
            grad = grad + dot(both.astype(BF), ret[a + 1, q * BLK : (q + 1) * BLK, :])
        tgrad[m] = grad.astype(BF)

    whole = rgs[...]
    wait(rgr.at[0:7], rg_r.at[0])
    for n in range(7):
        whole = whole + rgr[n]
    rg[...] = whole

    wait(snd.at[0:3, 0:288, :], a_s.at[0])
    wait(snd.at[:, 0:288, :], by_s.at[0])
    wait(G.at[0:3, 0:HALF, 0:896], z_s.at[0])
    wait(G.at[0:3, :, 0:1536], x_s.at[0])
    wait(G.at[:, :, 0:2048], d_s.at[0])
    wait(Pt.at[:, :, 0:1536], rx_s.at[0])
    wait(zr, rz_s.at[0])
    wait(ret.at[:, 0:288, :], b_s.at[0])
    wait(zr.at[0, 0:6], xb_s.at[0])
    wait(G.at[3, 0:HALF, 0:3584], z3_s.at[0])
    for k, half in enumerate((WgH.at[:, 0:HID], WuH.at[:, 0:HID], WdH.at[0:HID, :])):
        wait(half, w_s.at[k])
    wait(G.at[0, :, 0:1536], h_s.at[0])
    wait(arR, ar_s.at[0])
    wait(gts.at[0:7], gt_s.at[0])
    wait(dts.at[0:7], dt_s.at[0])
    wait(rgr.at[0:7], rg_s.at[0])


def write_out(*refs):
    sems = refs[12]
    copies = [pltpu.make_async_copy(refs[k], refs[6 + k], sems.at[k]) for k in range(6)]
    for copy in copies:
        copy.start()
    for copy in copies:
        copy.wait()


def shards(tokens, expert_ids, router_weight, w_gate, w_up, w_down, cotangent):
    big = lambda *dims: pltpu.VMEM(dims, BF)
    wide = lambda *dims: pltpu.VMEM(dims, F32)
    dma = lambda *dims: pltpu.SemaphoreType.DMA(dims)
    vm = pl.BlockSpec(memory_space=pltpu.VMEM)
    anyw = pl.BlockSpec(memory_space=pl.ANY)
    D = 4096
    results = pl.pallas_call(
        kernel,
        name="expert_layer",
        out_shape=(
            big(2, BLK, BLK), big(2, BLK, BLK), big(D, HID), big(D, HID), big(HID, D), wide(8, BLK),
        ),
        in_specs=[vm, vm, vm, vm, anyw, anyw, anyw],
        out_specs=(vm,) * 6,
        scratch_shapes=[
            big(4, ROWS, D),
            big(2048, 512), big(2048, 512), big(512, 2048), big(4, ROWS, BLK), big(4, 2, HALF, BLK), big(3, ROWS, BLK), big(4, 2, HALF, BLK),
            wide(ROWS, HID), wide(ROWS, HID), wide(ROWS, HID),
            big(2, ROWS, 512), big(2, ROWS, 512), big(2, ROWS, 512), big(2, ROWS, HID),
            wide(2, ROWS, BLK), wide(2, ROWS, BLK),
            big(4, ROWS, 2048), big(4, 4, ROWS, BLK), big(4, 4, ROWS, BLK), big(4, 4, ROWS, BLK),
            big(4, 8, HALF, BLK), big(4, 7, HALF, BLK), wide(4, 2, HALF, BLK), big(4, 2, HALF, BLK), big(4, ROWS, BLK),
            wide(2, 2, BLK, BLK), wide(2, 2, BLK, BLK), wide(2, BLK, BLK),
            wide(2, 3, 8, BLK), wide(2, 7, 8, BLK), wide(8, 8, BLK), wide(8, 8, BLK), wide(8, 8, BLK), wide(8, 8, BLK),
            wide(8, BLK), wide(7, 8, BLK),
            dma(6), dma(3), dma(3), dma(1), dma(3), dma(1), dma(3, 8), dma(1), dma(3, 8), dma(3, 8), dma(3),
            dma(1), dma(4), dma(1), dma(2, 3),
            dma(1), dma(4, 4), dma(4, 4), dma(4, 4), dma(1), dma(4), dma(1), dma(4),
            dma(1), dma(2, 3), dma(1), dma(1), dma(1), dma(1), dma(1), dma(1), dma(1), dma(4), dma(1), dma(4), dma(1), dma(4),
        ],
        compiler_params=pltpu.CompilerParams(
            collective_id=0, has_side_effects=True, vmem_limit_bytes=52 * 1024 * 1024
        ),
    )(tokens, cotangent, expert_ids.transpose(0, 2, 1), router_weight.T, w_gate[0], w_up[0], w_down[0])
    mixed, tgrad, gg, ug, dg, rg = pl.pallas_call(
        write_out,
        name="write_out",
        out_shape=tuple(jax.ShapeDtypeStruct(v.shape, v.dtype) for v in results),
        in_specs=[vm] * 6,
        out_specs=(anyw,) * 6,
        scratch_shapes=[dma(6)],
        compiler_params=pltpu.CompilerParams(vmem_limit_bytes=1024 * 1024),
    )(*(pltpu.with_memory_space_constraint(v, pltpu.VMEM) for v in results))
    return mixed, tgrad, gg[None], ug[None], dg[None], rg.T


def solution(mesh):
    split = Mesh(mesh.devices.reshape(4, 4, 2, 2, 4), REP + EP)
    in_specs = (
        P(None, EP, REP),
        P(None, EP, None),
        P(REP, None),
        P(EP, None, REP),
        P(EP, None, REP),
        P(EP, REP, None),
        P(None, EP, REP),
    )
    out_specs = (
        P(None, EP, REP),
        P(None, EP, REP),
        P(EP, None, REP),
        P(EP, None, REP),
        P(EP, REP, None),
        P(REP, None),
    )
    return jax.shard_map(shards, mesh=split, in_specs=in_specs, out_specs=out_specs, check_vma=False)
```
